32 devices in a mesh: seq: 16 (over z, y, core), head: 2 (over x).
Axes of the slice: x: 2, y: 2, z: 4, core: 2. Of those that a mesh axis runs over, the one named last changes fastest.
Arguments:
- teacher: bfloat16 [1, 4096, 4096], P(None, 'seq', 'head'), may hold values from -32 to 32
- student: bfloat16 [1, 4096, 1792], P(None, 'seq', 'head'), may hold values from -32 to 32
- weights: float32 [4096], P('seq'), may hold values from 1 to 32
Outputs:
- mean_loss: float32 [], replicated
- student_grad: float32 [1, 4096, 1792], P(None, 'seq', 'head')
The draws below stay inside these ranges and needn't reach their ends.
All inputs are finite; a program needn't handle non-finite values.
Results may differ from the reference program's by a relative error of at most 0.0011.
Values may be sent and summed in bfloat16 or wider, within the bound.
A program may use at most 128 MiB of HBM per device.

```python
import math
import jax
import jax.numpy as jnp
from jax import lax

TW = 256
SW = 112
HEADS = 16
RELS = 1
TOKENS = 4096


def clustered_base(key, salt, head_size):
    noise_key = jax.random.fold_in(key, salt)
    assign = jax.random.randint(jax.random.fold_in(key, 5), (RELS, TOKENS, HEADS), 0, 16)
    one_hot = (assign[..., None] == jnp.arange(16, dtype=jnp.int32)).astype(jnp.float32)
    centres = jnp.clip(jax.random.normal(jax.random.fold_in(noise_key, 21), (RELS, HEADS, 16, head_size), jnp.float32), -4.0, 4.0)
    placed = jnp.einsum('rthc,rhcd->rthd', one_hot, centres)
    noise = jnp.clip(jax.random.normal(jax.random.fold_in(noise_key, 1), (RELS, TOKENS, HEADS, head_size), jnp.float32), -4.0, 4.0)
    return (0.9 * placed + 0.45 * noise).reshape(RELS, TOKENS, HEADS * head_size)


def relation_vectors(key, salt, head_size):
    base = clustered_base(key, salt, head_size)
    values = jnp.clip(base * math.sqrt(0.5), -32.0, 32.0)
    return values.astype(jnp.bfloat16)


def draw_teacher(key, part):
    return relation_vectors(key, 11, TW)


def draw_student(key, part):
    return relation_vectors(key, 13, SW)


def draw_weights(key, part):
    position = jnp.arange(TOKENS, dtype=jnp.float32) / TOKENS
    return (1.0 + 3.0 * position) * jnp.exp(jax.random.uniform(key, (TOKENS,), jnp.float32, math.log(2.0), math.log(6.0)))


def setup_inputs(seed: int = 0) -> dict:
    keys = jax.random.split(jax.random.key(seed), 4)
    teacher = draw_teacher(jax.random.fold_in(keys[3], 71), 0)
    student = draw_student(jax.random.fold_in(keys[3], 71), 0)
    weights = draw_weights(jax.random.fold_in(keys[3], 71), 0)
    return dict(teacher=teacher, student=student, weights=weights)


def relation_pair(teach_rows, stud_rows, weights):
    teach_score = jnp.dot(teach_rows, teach_rows.T, preferred_element_type=jnp.float32) * (1.0 / math.sqrt(TW))
    stud_score = jnp.dot(stud_rows, stud_rows.T, preferred_element_type=jnp.float32) * (1.0 / math.sqrt(SW))
    teach_norm = jax.nn.logsumexp(teach_score, axis=1)
    stud_norm = jax.nn.logsumexp(stud_score, axis=1)
    teach_prob = jnp.exp(teach_score - teach_norm[:, None])
    stud_prob = jnp.exp(stud_score - stud_norm[:, None])
    divergence = lax.optimization_barrier(jnp.sum(teach_prob * (teach_score - stud_score), axis=1)) - teach_norm + stud_norm
    slopes = weights[:, None] * (stud_prob - teach_prob)
    slope_mix = (slopes + slopes.T).astype(jnp.bfloat16)
    gradient = jnp.dot(slope_mix, stud_rows, preferred_element_type=jnp.float32) * (1.0 / math.sqrt(SW))
    return (jnp.sum(weights * divergence), gradient)

def reference(teacher, student, weights):
    teach_heads = teacher.reshape(RELS, TOKENS, HEADS, TW).transpose(0, 2, 1, 3).reshape(RELS * HEADS, TOKENS, TW)
    stud_heads = student.reshape(RELS, TOKENS, HEADS, SW).transpose(0, 2, 1, 3).reshape(RELS * HEADS, TOKENS, SW)

    def single(stacked):
        return relation_pair(stacked[0], stacked[1], weights)
    totals, gradient = lax.map(single, (teach_heads, stud_heads))
    mean_loss = jnp.sum(totals) / (RELS * HEADS * TOKENS)
    student_grad = gradient.reshape(RELS, HEADS, TOKENS, SW).transpose(0, 2, 1, 3).reshape(RELS, TOKENS, HEADS * SW)
    return (mean_loss, student_grad)
```

```python
import functools
import math

import jax
import jax.numpy as jnp
from jax import lax
from jax.experimental import pallas as pl
from jax.experimental.pallas import tpu as pltpu
from jax.sharding import PartitionSpec as P

TW = 256
SW = 112
LANES = 128
SPAN = 119.0
LOG2E = math.log2(math.e)
LN2 = math.log(2.0)
NT = (((1,), (1,)), ((), ()))


def dot_nt(a, b):
    return lax.dot_general(a, b, NT, preferred_element_type=jnp.float32)


def kernel(
    heads, group, head_shards, t_in, s_in, w_in, grad_out, loss_out,
    u_in, w_tile, t_all, u_all, w_all, state, norms, grads, landed, losses, sums,
    t_send, u_send, w_send, t_fwd, u_fwd, t_recv, u_recv, w_recv, n_send, n_recv, g_send, g_recv,
    l_send, l_recv, s_send, s_recv,
):
    n = heads * group
    block = t_in.shape[0]
    me = lax.axis_index("seq")
    shard = lax.axis_index("head")
    head = lax.div(me, group)
    member = lax.rem(me, group)
    unroll = math.gcd(n, 8)
    pair = math.gcd(heads, 2)
    t_scale = LOG2E / math.sqrt(TW)
    u_scale = LOG2E / math.sqrt(SW)

    def other_head(i):
        return lax.rem(head + i, heads)

    def source_head(i):
        return lax.rem(head + heads - i, heads)

    def other_member(i):
        return lax.rem(member + i, group)

    def remote(src, dst, send, recv, device):
        target = device if isinstance(device, dict) else {"seq": device}
        return pltpu.make_async_remote_copy(
            src_ref=src, dst_ref=dst, send_sem=send, recv_sem=recv,
            device_id=target, device_id_type=pl.DeviceIdType.MESH,
        )

    def rows(slot):
        return pl.ds(pl.multiple_of(slot * block, block), block)

    def columns(h):
        return pl.ds(pl.multiple_of(h * TW, TW), TW)

    barrier = pltpu.get_barrier_semaphore()
    for i in range(1, n):
        pl.semaphore_signal(barrier, inc=1, device_id={"seq": lax.rem(me + i, n)}, device_id_type=pl.DeviceIdType.MESH)
    for i in range(1, head_shards):
        pl.semaphore_signal(barrier, inc=1, device_id={"head": lax.rem(shard + i, head_shards)}, device_id_type=pl.DeviceIdType.MESH)
    for h in range(heads):
        u_in[h] = jnp.concatenate(
            [s_in[:, h * SW:(h + 1) * SW], jnp.zeros((block, LANES - SW), jnp.bfloat16)], axis=1
        )
    w_tile[...] = jnp.broadcast_to(w_in[...], w_tile.shape)
    pl.semaphore_wait(barrier, n + head_shards - 2)

    direct = []
    for i in range(1, heads):
        h = other_head(i)
        device = h * group + member
        direct += [
            remote(t_in.at[:, columns(h)], t_all.at[rows(me)], t_send.at[i], t_recv.at[me], device),
            remote(u_in.at[h], u_all.at[rows(me)], u_send.at[i], u_recv.at[me], device),
            remote(w_tile, w_all.at[head], w_send.at[i], w_recv.at[head], device),
        ]
    for copy in direct:
        copy.start()

    def forwards(i, slot, t_src, u_src):
        pairs = []
        for g in range(1, group):
            device = head * group + other_member(g)
            pairs += [
                remote(t_src, t_all.at[rows(slot)], t_fwd.at[i, g], t_recv.at[slot], device),
                remote(u_src, u_all.at[rows(slot)], u_fwd.at[i, g], u_recv.at[slot], device),
            ]
        return pairs

    def arrived(slot):
        remote(t_in.at[:, columns(0)], t_all.at[rows(slot)], t_send.at[0], t_recv.at[slot], me).wait_recv()
        remote(u_in.at[0], u_all.at[rows(slot)], u_send.at[0], u_recv.at[slot], me).wait_recv()

    for copy in forwards(0, me, t_in.at[:, columns(head)], u_in.at[head]):
        copy.start()
    t_all[rows(me), :] = t_in[:, columns(head)]
    u_all[rows(me), :] = u_in[head]
    w_all[head] = w_tile[...]

    low = jnp.full((8, block), -1e30, jnp.float32)
    zero = jnp.zeros((8, block), jnp.float32)
    for h in range(heads):
        for k, value in enumerate((low, zero, zero, low, zero)):
            state[h, k] = value

    def tile(row_head, key_pair):
        t_own = t_all[rows(row_head * group + member), :]
        u_own = u_all[rows(row_head * group + member), :]
        width = math.gcd(group, 2)
        parts = [(a, q) for a in range(pair) for q in range(width)]

        def step(j, carry):
            t_max, t_sum, t_cross, u_max, u_sum = carry
            for a, q in parts:
                keys = rows(source_head(key_pair * pair + a) * group + j * width + q)
                t_score = (dot_nt(t_all[keys, :], t_own) * t_scale).reshape(block // 8, 8, block)
                u_score = (dot_nt(u_all[keys, :], u_own) * u_scale).reshape(block // 8, 8, block)
                t_top = jnp.maximum(t_max, jnp.max(t_score, axis=0))
                u_top = jnp.maximum(u_max, jnp.max(u_score, axis=0))
                t_exp = jnp.exp2(t_score - t_top[None])
                u_exp = jnp.exp2(u_score - u_top[None])
                t_keep = jnp.exp2(t_max - t_top)
                u_keep = jnp.exp2(u_max - u_top)
                t_sum = t_sum * t_keep + jnp.sum(t_exp, axis=0)
                t_cross = t_cross * t_keep + jnp.sum(t_exp * (t_score - u_score), axis=0)
                u_sum = u_sum * u_keep + jnp.sum(u_exp, axis=0)
                t_max, u_max = t_top, u_top
            return t_max, t_sum, t_cross, u_max, u_sum

        carry = tuple(state[row_head, k] for k in range(5))
        carry = step(0, carry) if group == width else lax.fori_loop(0, group // width, step, carry)
        for k in range(5):
            state[row_head, k] = carry[k]

    def arrival(p, carry):
        for a in range(pair):
            i = p * pair + a
            h = source_head(i)
            slot = h * group + member

            @pl.when(i > 0)
            def _(i=i, slot=slot):
                arrived(slot)
                for copy in forwards(i, slot, t_all.at[rows(slot)], u_all.at[rows(slot)]):
                    copy.start()
        for a in range(pair):
            h = source_head(p * pair + a)
            for g in range(1, group):
                arrived(h * group + other_member(g))

        def one(j, carry):
            old = j < p * pair
            fresh = j - p * pair
            tile(
                source_head(jnp.where(old, j, p * pair + lax.rem(fresh, pair))),
                jnp.where(old, p, lax.div(fresh, pair)),
            )
            return carry

        return lax.fori_loop(0, p * pair + (p + 1) * pair, one, carry)

    lax.fori_loop(0, heads // pair, arrival, 0)
    for i in range(1, heads):
        remote(w_tile, w_all.at[source_head(i)], w_send.at[0], w_recv.at[source_head(i)], me).wait_recv()

    loss = jnp.zeros((1, block), jnp.float32)
    for i in range(heads):
        t_max, t_sum, t_cross, u_max, u_sum = (state[i, k] for k in range(5))
        t_top = jnp.max(t_max, axis=0, keepdims=True)
        u_top = jnp.max(u_max, axis=0, keepdims=True)
        t_keep = jnp.exp2(t_max - t_top)
        t_total = jnp.sum(t_sum * t_keep, axis=0, keepdims=True)
        t_mixed = jnp.sum(t_cross * t_keep, axis=0, keepdims=True)
        u_total = jnp.sum(u_sum * jnp.exp2(u_max - u_top), axis=0, keepdims=True)
        t_norm = t_top + jnp.log(t_total) * LOG2E
        u_norm = u_top + jnp.log(u_total) * LOG2E
        weight = w_all[i][:1, :]
        weight_log = jnp.log(weight) * LOG2E
        norms[member, i, 0:8, :] = jnp.broadcast_to(t_norm - weight_log, (8, block))
        norms[member, i, 8:16, :] = jnp.broadcast_to(u_norm - weight_log, (8, block))
        loss = loss + weight * (t_mixed / t_total - t_norm + u_norm)
    loss = jnp.sum(loss, axis=1, keepdims=True) * (LN2 / (heads * head_shards * block * n))
    losses[me] = jnp.broadcast_to(loss, losses.shape[1:])
    stats = [
        remote(norms.at[member], norms.at[member], n_send.at[g], n_recv.at[member], head * group + other_member(g))
        for g in range(1, group)
    ]
    for i in range(1, n):
        stats.append(remote(losses.at[me], losses.at[me], l_send.at[i], l_recv.at[me], lax.rem(me + i, n)))
    for copy in stats:
        copy.start()
    for g in range(1, group):
        m = other_member(g)
        remote(norms.at[m], norms.at[m], n_send.at[0], n_recv.at[m], me).wait_recv()

    def row_grad(i):
        slot = i * group + member
        t_own = t_all[rows(slot), :]
        u_own = u_all[rows(slot), :]

        def own_norm(first):
            tall = jnp.broadcast_to(norms[member, i, first:first + 1, :], (LANES, block)).T
            return jnp.concatenate([tall] * (block // LANES), axis=1)

        t_mine = own_norm(0)
        u_mine = own_norm(8)

        def step(j, total):
            for q in range(unroll):
                key = j * unroll + q
                keys = rows(key)
                key_head = lax.div(key, group)
                key_member = lax.rem(key, group)
                t_theirs = norms[key_member, key_head, 0:1, :]
                u_theirs = norms[key_member, key_head, 8:9, :]
                u_keys = u_all[keys, :]
                t_score = dot_nt(t_own, t_all[keys, :]) * t_scale
                u_score = dot_nt(u_own, u_keys) * u_scale
                row_part = jnp.exp2(u_score - u_mine) - jnp.exp2(t_score - t_mine)
                col_part = jnp.exp2(u_score - u_theirs) - jnp.exp2(t_score - t_theirs)
                mix = (row_part + col_part).astype(jnp.bfloat16)
                total = total + jnp.dot(mix, u_keys, preferred_element_type=jnp.float32)
            return total

        total = lax.fori_loop(0, n // unroll, step, jnp.zeros((block, LANES), jnp.float32))
        return total * (1.0 / math.sqrt(SW))

    def send_grad(i, h):
        return remote(grads.at[h], landed.at[head], g_send.at[h], g_recv.at[head], h * group + member)

    def grad_step(i, carry):
        h = other_head(i)
        grads[h] = row_grad(h)
        send_grad(i, h).start()
        return carry

    lax.fori_loop(1, heads, grad_step, 0)
    for i in range(1, n):
        peer = lax.rem(me + i, n)
        remote(losses.at[peer], losses.at[peer], l_send.at[0], l_recv.at[peer], me).wait_recv()
    sums[shard] = jnp.sum(losses[...], axis=0)
    shards = [
        remote(sums.at[shard], sums.at[shard], s_send.at[i], s_recv.at[shard], {"head": lax.rem(shard + i, head_shards)})
        for i in range(1, head_shards)
    ]
    for copy in shards:
        copy.start()
    landed[head] = row_grad(head)
    for i in range(1, head_shards):
        peer = lax.rem(shard + i, head_shards)
        remote(sums.at[peer], sums.at[peer], s_send.at[0], s_recv.at[peer], {"head": peer}).wait_recv()
    loss_out[...] = jnp.sum(sums[...], axis=0)

    for copy in direct + stats + shards:
        copy.wait_send()
    for i in range(heads):
        for copy in forwards(i, me, t_in.at[:, columns(0)], u_in.at[0]):
            copy.wait_send()
    for i in range(1, heads):
        send_grad(i, other_head(i)).wait_send()
    for h in range(heads):
        @pl.when(head != h)
        def _(h=h):
            remote(grads.at[h], landed.at[h], g_send.at[h], g_recv.at[h], me).wait_recv()
        grad_out[:, h * SW:(h + 1) * SW] = landed[h][:, :SW]


def pair_kernel(
    heads, head_shards, t_in, s_in, w_in, grad_out, loss_out,
    u_in, w_tile, t_all, u_all, u_turn, w_all, t_raw, u_raw, t_exp, u_exp, t_refs, u_refs, t_top, u_top, cross,
    t_rows, u_rows, parts, landed_parts, grads, code_out, code_in, landed, losses, sums,
    t_send, u_send, w_send, t_fwd, u_fwd, t_recv, u_recv, w_recv, p_send, p_recv, g_send, g_recv,
    l_send, l_recv, s_send, s_recv,
):
    group = 2
    n = heads * group
    block = t_in.shape[0]
    both = group * block
    me = lax.axis_index("seq")
    shard = lax.axis_index("head")
    head = lax.div(me, group)
    member = lax.rem(me, group)
    mate = head * group + 1 - member
    bits = (heads - 1).bit_length()
    t_scale = LOG2E / math.sqrt(TW)
    u_scale = LOG2E / math.sqrt(SW)

    def flip(i):
        out = 0
        for k in range(bits):
            out = out + lax.rem(lax.div(head, 2**k) + lax.div(jnp.int32(i), 2**k), 2) * 2**k
        return out

    def remote(src, dst, send, recv, device):
        target = device if isinstance(device, dict) else {"seq": device}
        return pltpu.make_async_remote_copy(
            src_ref=src, dst_ref=dst, send_sem=send, recv_sem=recv,
            device_id=target, device_id_type=pl.DeviceIdType.MESH,
        )

    def rows(slot):
        return pl.ds(pl.multiple_of(slot * block, block), block)

    def both_rows(h):
        return pl.ds(pl.multiple_of(h * both, both), both)

    def head_rows(h):
        return pl.ds(pl.multiple_of(h * SW, 16), SW)

    def columns(h):
        return pl.ds(pl.multiple_of(h * TW, TW), TW)

    barrier = pltpu.get_barrier_semaphore()
    for i in range(1, n):
        pl.semaphore_signal(barrier, inc=1, device_id={"seq": lax.rem(me + i, n)}, device_id_type=pl.DeviceIdType.MESH)
    for i in range(1, head_shards):
        pl.semaphore_signal(barrier, inc=1, device_id={"head": lax.rem(shard + i, head_shards)}, device_id_type=pl.DeviceIdType.MESH)
    for c in range(heads * SW // LANES):
        piece = s_in[:, c * LANES:(c + 1) * LANES].astype(jnp.float32)
        u_in[c * LANES:(c + 1) * LANES, :] = piece.T.astype(jnp.bfloat16)
    spare = lax.broadcasted_iota(jnp.int32, (LANES - SW, block), 0)
    ones = jnp.where(spare == 0, 1.0, 0.0).astype(jnp.bfloat16)
    for k in range(n):
        u_turn[k, SW:, :] = ones
    w_tile[...] = jnp.broadcast_to(w_in[...], w_tile.shape)
    pl.semaphore_wait(barrier, n + head_shards - 2)

    direct = []
    for i in range(1, heads):
        h = flip(i)
        device = h * group + member
        direct += [
            remote(t_in.at[:, columns(h)], t_all.at[rows(me)], t_send.at[i], t_recv.at[me], device),
            remote(u_in.at[head_rows(h)], u_turn.at[me, pl.ds(0, SW)], u_send.at[i], u_recv.at[me], device),
            remote(w_tile, w_all.at[head], w_send.at[i], w_recv.at[head], device),
        ]
    for copy in direct:
        copy.start()

    def forwards(i, slot, t_src, u_src):
        return [
            remote(t_src, t_all.at[rows(slot)], t_fwd.at[i], t_recv.at[slot], mate),
            remote(u_src, u_turn.at[slot, pl.ds(0, SW)], u_fwd.at[i], u_recv.at[slot], mate),
        ]

    def arrived(slot):
        remote(t_in.at[:, columns(0)], t_all.at[rows(slot)], t_send.at[0], t_recv.at[slot], mate).wait_recv()
        remote(u_in.at[head_rows(0)], u_turn.at[slot, pl.ds(0, SW)], u_send.at[0], u_recv.at[slot], mate).wait_recv()

    for copy in forwards(0, me, t_in.at[:, columns(head)], u_in.at[head_rows(head)]):
        copy.start()
    t_all[rows(me), :] = t_in[:, columns(head)]
    u_turn[me, :SW, :] = u_in[head_rows(head), :]
    w_all[head] = w_tile[...]
    lane = lax.broadcasted_iota(jnp.int32, (block, LANES), 1)

    def turn_u(slot):
        u_all[rows(slot), :] = jnp.where(lane < SW, u_turn[slot].astype(jnp.float32).T, 0.0).astype(jnp.bfloat16)

    for h in range(heads):
        t_top[h] = jnp.full((8, block), -1e30, jnp.float32)
        u_top[h] = jnp.full((8, block), -1e30, jnp.float32)
        cross[h] = jnp.zeros((8, block), jnp.float32)
        t_rows[h] = jnp.zeros((LANES, block), jnp.float32)
        u_rows[h] = jnp.zeros((LANES, block), jnp.float32)

    def fold(x, op):
        return op(x.reshape(x.shape[0] // 8, 8, block), axis=0)

    def unit(i, k):
        early = k < i
        return flip(jnp.where(early, i, k - i)), flip(jnp.where(early, k, i))

    def scores(i, k, b):
        own, key = unit(i, k)
        slot = own * group + member
        t = dot_nt(t_all[both_rows(key), :], t_all[rows(slot), :])
        u = jnp.dot(u_all[both_rows(key), :], u_turn[slot], preferred_element_type=jnp.float32)
        t_raw[b] = t
        u_raw[b] = u
        return fold(t, jnp.max), fold(u, jnp.max)

    def soften(i, k, b, peaks):
        own, key = unit(i, k)

        def side(raw_ref, peak, scale, top, refs, exps, out, with_cross):
            raw = raw_ref[b]
            old = top[own]
            new = jnp.maximum(old, jnp.max(peak, axis=0, keepdims=True))
            top[own] = new
            refs[own, pl.ds(key, 1), :] = new[:1] * scale
            value = jnp.exp2(raw * scale - new[:1] * scale).astype(jnp.bfloat16)
            keep = jnp.exp2((old - new) * scale)
            if with_cross:
                cross[own] = cross[own] * keep + fold(value.astype(jnp.float32) * raw, jnp.sum)
            total = out[own] * keep[:1]
            for q in range(group):
                piece = value[q * block:(q + 1) * block]
                exps[own, key * group + q] = piece
                total = total + jnp.dot(u_turn[key * group + q], piece, preferred_element_type=jnp.float32)
            out[own] = total

        side(t_raw, peaks[0], t_scale, t_top, t_refs, t_exp, t_rows, True)
        side(u_raw, peaks[1], u_scale, u_top, u_refs, u_exp, u_rows, False)

    turn_u(me)
    arrived(head * group + 1 - member)
    turn_u(head * group + 1 - member)
    soften(0, 0, 0, scores(0, 0, 0))

    def arrival(i, carry):
        h = flip(i)
        slot = h * group + member
        other = h * group + 1 - member
        arrived(slot)
        for copy in forwards(i, slot, t_all.at[rows(slot)], u_turn.at[slot, pl.ds(0, SW)]):
            copy.start()
        turn_u(slot)

        def two(j, peaks):
            @pl.when(j == lax.div(i - 1, 2))
            def _():
                arrived(other)
                turn_u(other)
            k = 2 * j
            later = scores(i, k + 1, 1)
            soften(i, k, 0, peaks)
            peaks = scores(i, k + 2, 0)
            soften(i, k + 1, 1, later)
            return peaks

        soften(i, 2 * i, 0, lax.fori_loop(0, i, two, scores(i, 0, 0)))
        return carry

    lax.fori_loop(1, heads, arrival, 0)
    for i in range(1, heads):
        remote(w_tile, w_all.at[flip(i)], w_send.at[0], w_recv.at[flip(i)], mate).wait_recv()

    loss = jnp.zeros((1, block), jnp.float32)
    for h in range(heads):
        weight = w_all[h][:1, :]
        t_sum = t_rows[h, SW:SW + 1, :]
        u_sum = u_rows[h, SW:SW + 1, :]
        t_norm = t_top[h][:1] * t_scale + jnp.log(t_sum) * LOG2E
        u_norm = u_top[h][:1] * u_scale + jnp.log(u_sum) * LOG2E
        own_u = u_turn[h * group + member].astype(jnp.float32)[:SW]
        seen = jnp.sum(own_u * t_rows[h, :SW, :], axis=0, keepdims=True) * u_scale
        mean = (jnp.sum(cross[h], axis=0, keepdims=True) * t_scale - seen) / t_sum
        loss = loss + weight * (mean - t_norm + u_norm)
        t_part = weight / t_sum
        u_part = weight / u_sum
        t_last = t_top[h][:1] * t_scale
        u_last = u_top[h][:1] * u_scale
        t_refs[h] = jnp.exp2(t_refs[h] - t_last) * t_part
        u_refs[h] = jnp.exp2(u_refs[h] - u_last) * u_part
        u_rows[h] = u_rows[h] * u_part - t_rows[h] * t_part
    loss = jnp.sum(loss, axis=1, keepdims=True) * (LN2 / (heads * head_shards * block * n))
    losses[me] = jnp.broadcast_to(loss, losses.shape[1:])
    stats = [
        remote(losses.at[me], losses.at[me], l_send.at[i], l_recv.at[me], lax.rem(me + i, n))
        for i in range(1, n)
    ]
    for copy in stats:
        copy.start()

    def column_part(h, q):
        key = h * group + q
        total = jnp.zeros((LANES, block), jnp.float32)
        for own in range(heads):
            t_part = t_exp[own, key].astype(jnp.float32) * t_refs[own, pl.ds(h, 1), :]
            u_part = u_exp[own, key].astype(jnp.float32) * u_refs[own, pl.ds(h, 1), :]
            total = total + dot_nt(u_turn[own * group + member], (u_part - t_part).astype(jnp.bfloat16))
        return total[:SW]

    def swap(h):
        return remote(parts.at[h], landed_parts.at[h], p_send.at[h], p_recv.at[h], mate)

    def give(i, h):
        return remote(code_out.at[h], code_in.at[head], g_send.at[i], g_recv.at[head], h * group + member)

    def finish(h):
        swap(h).wait_recv()
        return (grads[h] + landed_parts[h]) * (1.0 / math.sqrt(SW))

    def hand_over(i):
        h = flip(i)
        grad = finish(h)
        peak = jnp.maximum(jnp.max(jnp.abs(grad), axis=0, keepdims=True), 1e-30)
        peak = (peak * 1.01).astype(jnp.bfloat16)
        code_out[h, SW:, :] = jnp.broadcast_to(peak, (LANES - SW, block))
        code_out[h, :SW, :] = jnp.exp2(grad * (SPAN / peak.astype(jnp.float32))).astype(jnp.bfloat16)
        give(i, h).start()

    def step(j, carry):
        i = heads - 1 - j
        h = flip(i)
        parts[h] = column_part(h, 1 - member)
        swap(h).start()

        @pl.when(j > 0)
        def _():
            hand_over(i + 1)
        grads[h] = column_part(h, member) + u_rows[h, :SW, :]
        return carry

    lax.fori_loop(0, heads, step, 0)
    for i in range(1, n):
        peer = lax.rem(me + i, n)
        remote(losses.at[peer], losses.at[peer], l_send.at[0], l_recv.at[peer], mate).wait_recv()
    sums[shard] = jnp.sum(losses[...], axis=0)
    shards = [
        remote(sums.at[shard], sums.at[shard], s_send.at[i], s_recv.at[shard], {"head": lax.rem(shard + i, head_shards)})
        for i in range(1, head_shards)
    ]
    for copy in shards:
        copy.start()
    landed[head_rows(head), :] = finish(head)
    for i in range(1, head_shards):
        peer = lax.rem(shard + i, head_shards)
        remote(sums.at[peer], sums.at[peer], s_send.at[0], s_recv.at[peer], {"head": peer}).wait_recv()
    loss_out[...] = jnp.sum(sums[...], axis=0)

    for copy in direct + stats + shards:
        copy.wait_send()
    for i in range(heads):
        for copy in forwards(i, me, t_in.at[:, columns(0)], u_in.at[head_rows(0)]):
            copy.wait_send()
        swap(flip(i)).wait_send()
    for i in range(1, heads):
        give(i, flip(i)).wait_send()
    for i in range(1, heads):
        h = flip(i)
        remote(code_out.at[h], code_in.at[h], g_send.at[0], g_recv.at[h], mate).wait_recv()
        code = code_in[h].astype(jnp.float32)
        landed[head_rows(h), :] = jnp.log(code[:SW]) * (code[SW:SW + 1] * (LOG2E / SPAN))
    for c in range(heads * SW // LANES):
        grad_out[:, c * LANES:(c + 1) * LANES] = landed[c * LANES:(c + 1) * LANES, :].T

def pair_call(heads, n, head_shards, block):
    vmem = pl.BlockSpec(memory_space=pltpu.VMEM)
    dma = pltpu.SemaphoreType.DMA
    f32, bf16 = jnp.float32, jnp.bfloat16
    return pl.pallas_call(
        functools.partial(pair_kernel, heads, head_shards),
        out_shape=(
            jax.ShapeDtypeStruct((block, heads * SW), f32),
            jax.ShapeDtypeStruct((8, LANES), f32),
        ),
        in_specs=[vmem] * 3,
        out_specs=(vmem, vmem),
        scratch_shapes=[
            pltpu.VMEM((heads * SW, block), bf16),
            pltpu.VMEM((8, block), f32),
            pltpu.VMEM((n * block, TW), bf16),
            pltpu.VMEM((n * block, LANES), bf16),
            pltpu.VMEM((n, LANES, block), bf16),
            pltpu.VMEM((heads, 8, block), f32),
            pltpu.VMEM((2, 2 * block, block), f32),
            pltpu.VMEM((2, 2 * block, block), f32),
            pltpu.VMEM((heads, n, block, block), bf16),
            pltpu.VMEM((heads, n, block, block), bf16),
            pltpu.VMEM((heads, heads, block), f32),
            pltpu.VMEM((heads, heads, block), f32),
            pltpu.VMEM((heads, 8, block), f32),
            pltpu.VMEM((heads, 8, block), f32),
            pltpu.VMEM((heads, 8, block), f32),
            pltpu.VMEM((heads, LANES, block), f32),
            pltpu.VMEM((heads, LANES, block), f32),
            pltpu.VMEM((heads, SW, block), f32),
            pltpu.VMEM((heads, SW, block), f32),
            pltpu.VMEM((heads, SW, block), f32),
            pltpu.VMEM((heads, LANES, block), bf16),
            pltpu.VMEM((heads, LANES, block), bf16),
            pltpu.VMEM((heads * SW, block), f32),
            pltpu.VMEM((n, 8, LANES), f32),
            pltpu.VMEM((head_shards, 8, LANES), f32),
            dma((heads,)), dma((heads,)), dma((heads,)),
            dma((heads,)), dma((heads,)),
            dma((n,)), dma((n,)), dma((heads,)),
            dma((heads,)), dma((heads,)),
            dma((heads,)), dma((heads,)),
            dma((n,)), dma((n,)), dma((head_shards,)), dma((head_shards,)),
        ],
        compiler_params=pltpu.CompilerParams(
            collective_id=1, has_side_effects=True, vmem_limit_bytes=60 * 2**20
        ),
    )


def local(teacher, student, weights):
    relations, block, t_columns = teacher.shape
    assert relations == 1
    heads = t_columns // TW
    n = lax.axis_size("seq")
    head_shards = lax.axis_size("head")
    assert n % heads == 0
    group = n // heads
    if group == 2 and heads & (heads - 1) == 0 and heads * SW % LANES == 0 and n * n * block * block <= 2**24:
        student_grad, loss = pair_call(heads, n, head_shards, block)(teacher[0], student[0], weights[None, :])
        return (loss[0, 0], student_grad[None])
    vmem = pl.BlockSpec(memory_space=pltpu.VMEM)
    dma = pltpu.SemaphoreType.DMA
    student_grad, loss = pl.pallas_call(
        functools.partial(kernel, heads, group, head_shards),
        out_shape=(
            jax.ShapeDtypeStruct((block, heads * SW), jnp.float32),
            jax.ShapeDtypeStruct((8, LANES), jnp.float32),
        ),
        in_specs=[vmem] * 3,
        out_specs=(vmem, vmem),
        scratch_shapes=[
            pltpu.VMEM((heads, block, LANES), jnp.bfloat16),
            pltpu.VMEM((8, block), jnp.float32),
            pltpu.VMEM((n * block, TW), jnp.bfloat16),
            pltpu.VMEM((n * block, LANES), jnp.bfloat16),
            pltpu.VMEM((heads, 8, block), jnp.float32),
            pltpu.VMEM((heads, 5, 8, block), jnp.float32),
            pltpu.VMEM((group, heads, 16, block), jnp.float32),
            pltpu.VMEM((heads, block, LANES), jnp.float32),
            pltpu.VMEM((heads, block, LANES), jnp.float32),
            pltpu.VMEM((n, 8, LANES), jnp.float32),
            pltpu.VMEM((head_shards, 8, LANES), jnp.float32),
            dma((heads,)), dma((heads,)), dma((heads,)),
            dma((heads, group)), dma((heads, group)),
            dma((n,)), dma((n,)), dma((heads,)),
            dma((group,)), dma((group,)),
            dma((heads,)), dma((heads,)),
            dma((n,)), dma((n,)), dma((head_shards,)), dma((head_shards,)),
        ],
        compiler_params=pltpu.CompilerParams(
            collective_id=0, has_side_effects=True, vmem_limit_bytes=60 * 2**20
        ),
    )(teacher[0], student[0], weights[None, :])
    return (loss[0, 0], student_grad[None])


def solution(mesh):
    return jax.shard_map(
        local,
        mesh=mesh,
        in_specs=(P(None, "seq", "head"), P(None, "seq", "head"), P("seq")),
        out_specs=(P(), P(None, "seq", "head")),
        check_vma=False,
    )
```

```python
import functools
import math

import jax
import jax.numpy as jnp
from jax import lax
from jax.experimental import pallas as pl
from jax.experimental.pallas import tpu as pltpu
from jax.sharding import PartitionSpec as P

TW = 256
SW = 112
LANES = 128
SPAN = 119.0
LOG2E = math.log2(math.e)
LN2 = math.log(2.0)
NT = (((1,), (1,)), ((), ()))


def dot_nt(a, b):
    return lax.dot_general(a, b, NT, preferred_element_type=jnp.float32)


def kernel(
    heads, group, head_shards, t_in, s_in, w_in, grad_out, loss_out,
    u_in, w_tile, t_all, u_all, w_all, state, norms, grads, landed, losses, sums,
    t_send, u_send, w_send, t_fwd, u_fwd, t_recv, u_recv, w_recv, n_send, n_recv, g_send, g_recv,
    l_send, l_recv, s_send, s_recv,
):
    n = heads * group
    block = t_in.shape[0]
    me = lax.axis_index("seq")
    shard = lax.axis_index("head")
    head = lax.div(me, group)
    member = lax.rem(me, group)
    unroll = math.gcd(n, 8)
    pair = math.gcd(heads, 2)
    t_scale = LOG2E / math.sqrt(TW)
    u_scale = LOG2E / math.sqrt(SW)

    def other_head(i):
        return lax.rem(head + i, heads)

    def source_head(i):
        return lax.rem(head + heads - i, heads)

    def other_member(i):
        return lax.rem(member + i, group)

    def remote(src, dst, send, recv, device):
        target = device if isinstance(device, dict) else {"seq": device}
        return pltpu.make_async_remote_copy(
            src_ref=src, dst_ref=dst, send_sem=send, recv_sem=recv,
            device_id=target, device_id_type=pl.DeviceIdType.MESH,
        )

    def rows(slot):
        return pl.ds(pl.multiple_of(slot * block, block), block)

    def columns(h):
        return pl.ds(pl.multiple_of(h * TW, TW), TW)

    barrier = pltpu.get_barrier_semaphore()
    for i in range(1, n):
        pl.semaphore_signal(barrier, inc=1, device_id={"seq": lax.rem(me + i, n)}, device_id_type=pl.DeviceIdType.MESH)
    for i in range(1, head_shards):
        pl.semaphore_signal(barrier, inc=1, device_id={"head": lax.rem(shard + i, head_shards)}, device_id_type=pl.DeviceIdType.MESH)
    for h in range(heads):
        u_in[h] = jnp.concatenate(
            [s_in[:, h * SW:(h + 1) * SW], jnp.zeros((block, LANES - SW), jnp.bfloat16)], axis=1
        )
    w_tile[...] = jnp.broadcast_to(w_in[...], w_tile.shape)
    pl.semaphore_wait(barrier, n + head_shards - 2)

    direct = []
    for i in range(1, heads):
        h = other_head(i)
        device = h * group + member
        direct += [
            remote(t_in.at[:, columns(h)], t_all.at[rows(me)], t_send.at[i], t_recv.at[me], device),
            remote(u_in.at[h], u_all.at[rows(me)], u_send.at[i], u_recv.at[me], device),
            remote(w_tile, w_all.at[head], w_send.at[i], w_recv.at[head], device),
        ]
    for copy in direct:
        copy.start()

    def forwards(i, slot, t_src, u_src):
        pairs = []
        for g in range(1, group):
            device = head * group + other_member(g)
            pairs += [
                remote(t_src, t_all.at[rows(slot)], t_fwd.at[i, g], t_recv.at[slot], device),
                remote(u_src, u_all.at[rows(slot)], u_fwd.at[i, g], u_recv.at[slot], device),
            ]
        return pairs

    def arrived(slot):
        remote(t_in.at[:, columns(0)], t_all.at[rows(slot)], t_send.at[0], t_recv.at[slot], me).wait_recv()
        remote(u_in.at[0], u_all.at[rows(slot)], u_send.at[0], u_recv.at[slot], me).wait_recv()

    for copy in forwards(0, me, t_in.at[:, columns(head)], u_in.at[head]):
        copy.start()
    t_all[rows(me), :] = t_in[:, columns(head)]
    u_all[rows(me), :] = u_in[head]
    w_all[head] = w_tile[...]

    low = jnp.full((8, block), -1e30, jnp.float32)
    zero = jnp.zeros((8, block), jnp.float32)
    for h in range(heads):
        for k, value in enumerate((low, zero, zero, low, zero)):
            state[h, k] = value

    def tile(row_head, key_pair):
        t_own = t_all[rows(row_head * group + member), :]
        u_own = u_all[rows(row_head * group + member), :]
        width = math.gcd(group, 2)
        parts = [(a, q) for a in range(pair) for q in range(width)]

        def step(j, carry):
            t_max, t_sum, t_cross, u_max, u_sum = carry
            for a, q in parts:
                keys = rows(source_head(key_pair * pair + a) * group + j * width + q)
                t_score = (dot_nt(t_all[keys, :], t_own) * t_scale).reshape(block // 8, 8, block)
                u_score = (dot_nt(u_all[keys, :], u_own) * u_scale).reshape(block // 8, 8, block)
                t_top = jnp.maximum(t_max, jnp.max(t_score, axis=0))
                u_top = jnp.maximum(u_max, jnp.max(u_score, axis=0))
                t_exp = jnp.exp2(t_score - t_top[None])
                u_exp = jnp.exp2(u_score - u_top[None])
                t_keep = jnp.exp2(t_max - t_top)
                u_keep = jnp.exp2(u_max - u_top)
                t_sum = t_sum * t_keep + jnp.sum(t_exp, axis=0)
                t_cross = t_cross * t_keep + jnp.sum(t_exp * (t_score - u_score), axis=0)
                u_sum = u_sum * u_keep + jnp.sum(u_exp, axis=0)
                t_max, u_max = t_top, u_top
            return t_max, t_sum, t_cross, u_max, u_sum

        carry = tuple(state[row_head, k] for k in range(5))
        carry = step(0, carry) if group == width else lax.fori_loop(0, group // width, step, carry)
        for k in range(5):
            state[row_head, k] = carry[k]

    def arrival(p, carry):
        for a in range(pair):
            i = p * pair + a
            h = source_head(i)
            slot = h * group + member

            @pl.when(i > 0)
            def _(i=i, slot=slot):
                arrived(slot)
                for copy in forwards(i, slot, t_all.at[rows(slot)], u_all.at[rows(slot)]):
                    copy.start()
        for a in range(pair):
            h = source_head(p * pair + a)
            for g in range(1, group):
                arrived(h * group + other_member(g))

        def one(j, carry):
            old = j < p * pair
            fresh = j - p * pair
            tile(
                source_head(jnp.where(old, j, p * pair + lax.rem(fresh, pair))),
                jnp.where(old, p, lax.div(fresh, pair)),
            )
            return carry

        return lax.fori_loop(0, p * pair + (p + 1) * pair, one, carry)

    lax.fori_loop(0, heads // pair, arrival, 0)
    for i in range(1, heads):
        remote(w_tile, w_all.at[source_head(i)], w_send.at[0], w_recv.at[source_head(i)], me).wait_recv()

    loss = jnp.zeros((1, block), jnp.float32)
    for i in range(heads):
        t_max, t_sum, t_cross, u_max, u_sum = (state[i, k] for k in range(5))
        t_top = jnp.max(t_max, axis=0, keepdims=True)
        u_top = jnp.max(u_max, axis=0, keepdims=True)
        t_keep = jnp.exp2(t_max - t_top)
        t_total = jnp.sum(t_sum * t_keep, axis=0, keepdims=True)
        t_mixed = jnp.sum(t_cross * t_keep, axis=0, keepdims=True)
        u_total = jnp.sum(u_sum * jnp.exp2(u_max - u_top), axis=0, keepdims=True)
        t_norm = t_top + jnp.log(t_total) * LOG2E
        u_norm = u_top + jnp.log(u_total) * LOG2E
        weight = w_all[i][:1, :]
        weight_log = jnp.log(weight) * LOG2E
        norms[member, i, 0:8, :] = jnp.broadcast_to(t_norm - weight_log, (8, block))
        norms[member, i, 8:16, :] = jnp.broadcast_to(u_norm - weight_log, (8, block))
        loss = loss + weight * (t_mixed / t_total - t_norm + u_norm)
    loss = jnp.sum(loss, axis=1, keepdims=True) * (LN2 / (heads * head_shards * block * n))
    losses[me] = jnp.broadcast_to(loss, losses.shape[1:])
    stats = [
        remote(norms.at[member], norms.at[member], n_send.at[g], n_recv.at[member], head * group + other_member(g))
        for g in range(1, group)
    ]
    for i in range(1, n):
        stats.append(remote(losses.at[me], losses.at[me], l_send.at[i], l_recv.at[me], lax.rem(me + i, n)))
    for copy in stats:
        copy.start()
    for g in range(1, group):
        m = other_member(g)
        remote(norms.at[m], norms.at[m], n_send.at[0], n_recv.at[m], me).wait_recv()

    def row_grad(i):
        slot = i * group + member
        t_own = t_all[rows(slot), :]
        u_own = u_all[rows(slot), :]

        def own_norm(first):
            tall = jnp.broadcast_to(norms[member, i, first:first + 1, :], (LANES, block)).T
            return jnp.concatenate([tall] * (block // LANES), axis=1)

        t_mine = own_norm(0)
        u_mine = own_norm(8)

        def step(j, total):
            for q in range(unroll):
                key = j * unroll + q
                keys = rows(key)
                key_head = lax.div(key, group)
                key_member = lax.rem(key, group)
                t_theirs = norms[key_member, key_head, 0:1, :]
                u_theirs = norms[key_member, key_head, 8:9, :]
                u_keys = u_all[keys, :]
                t_score = dot_nt(t_own, t_all[keys, :]) * t_scale
                u_score = dot_nt(u_own, u_keys) * u_scale
                row_part = jnp.exp2(u_score - u_mine) - jnp.exp2(t_score - t_mine)
                col_part = jnp.exp2(u_score - u_theirs) - jnp.exp2(t_score - t_theirs)
                mix = (row_part + col_part).astype(jnp.bfloat16)
                total = total + jnp.dot(mix, u_keys, preferred_element_type=jnp.float32)
            return total

        total = lax.fori_loop(0, n // unroll, step, jnp.zeros((block, LANES), jnp.float32))
        return total * (1.0 / math.sqrt(SW))

    def send_grad(i, h):
        return remote(grads.at[h], landed.at[head], g_send.at[h], g_recv.at[head], h * group + member)

    def grad_step(i, carry):
        h = other_head(i)
        grads[h] = row_grad(h)
        send_grad(i, h).start()
        return carry

    lax.fori_loop(1, heads, grad_step, 0)
    for i in range(1, n):
        peer = lax.rem(me + i, n)
        remote(losses.at[peer], losses.at[peer], l_send.at[0], l_recv.at[peer], me).wait_recv()
    sums[shard] = jnp.sum(losses[...], axis=0)
    shards = [
        remote(sums.at[shard], sums.at[shard], s_send.at[i], s_recv.at[shard], {"head": lax.rem(shard + i, head_shards)})
        for i in range(1, head_shards)
    ]
    for copy in shards:
        copy.start()
    landed[head] = row_grad(head)
    for i in range(1, head_shards):
        peer = lax.rem(shard + i, head_shards)
        remote(sums.at[peer], sums.at[peer], s_send.at[0], s_recv.at[peer], {"head": peer}).wait_recv()
    loss_out[...] = jnp.sum(sums[...], axis=0)

    for copy in direct + stats + shards:
        copy.wait_send()
    for i in range(heads):
        for copy in forwards(i, me, t_in.at[:, columns(0)], u_in.at[0]):
            copy.wait_send()
    for i in range(1, heads):
        send_grad(i, other_head(i)).wait_send()
    for h in range(heads):
        @pl.when(head != h)
        def _(h=h):
            remote(grads.at[h], landed.at[h], g_send.at[h], g_recv.at[h], me).wait_recv()
        grad_out[:, h * SW:(h + 1) * SW] = landed[h][:, :SW]


def pair_kernel(
    heads, head_shards, t_in, s_in, w_in, code_in, loss_out,
    u_in, w_tile, t_all, u_all, u_turn, w_all, t_raw, u_raw, t_exp, u_exp, t_refs, u_refs, t_top, u_top, cross,
    t_rows, u_rows, parts, landed_parts, grads, code_out, losses, sums,
    t_send, u_send, w_send, t_fwd, u_fwd, t_recv, u_recv, w_recv, p_send, p_recv, g_send, g_recv,
    l_send, l_recv, s_send, s_recv, own_sem,
):
    group = 2
    n = heads * group
    block = t_in.shape[0]
    both = group * block
    me = lax.axis_index("seq")
    shard = lax.axis_index("head")
    head = lax.div(me, group)
    member = lax.rem(me, group)
    mate = head * group + 1 - member
    bits = (heads - 1).bit_length()
    t_scale = LOG2E / math.sqrt(TW)
    u_scale = LOG2E / math.sqrt(SW)

    def flip(i):
        out = 0
        for k in range(bits):
            out = out + lax.rem(lax.div(head, 2**k) + lax.div(jnp.int32(i), 2**k), 2) * 2**k
        return out

    def remote(src, dst, send, recv, device):
        target = device if isinstance(device, dict) else {"seq": device}
        return pltpu.make_async_remote_copy(
            src_ref=src, dst_ref=dst, send_sem=send, recv_sem=recv,
            device_id=target, device_id_type=pl.DeviceIdType.MESH,
        )

    def rows(slot):
        return pl.ds(pl.multiple_of(slot * block, block), block)

    def both_rows(h):
        return pl.ds(pl.multiple_of(h * both, both), both)

    def head_rows(h):
        return pl.ds(pl.multiple_of(h * SW, 16), SW)

    def columns(h):
        return pl.ds(pl.multiple_of(h * TW, TW), TW)

    barrier = pltpu.get_barrier_semaphore()
    for i in range(1, n):
        pl.semaphore_signal(barrier, inc=1, device_id={"seq": lax.rem(me + i, n)}, device_id_type=pl.DeviceIdType.MESH)
    for i in range(1, head_shards):
        pl.semaphore_signal(barrier, inc=1, device_id={"head": lax.rem(shard + i, head_shards)}, device_id_type=pl.DeviceIdType.MESH)
    for c in range(heads * SW // LANES):
        piece = s_in[:, c * LANES:(c + 1) * LANES].astype(jnp.float32)
        u_in[c * LANES:(c + 1) * LANES, :] = piece.T.astype(jnp.bfloat16)
    spare = lax.broadcasted_iota(jnp.int32, (LANES - SW, block), 0)
    ones = jnp.where(spare == 0, 1.0, 0.0).astype(jnp.bfloat16)
    for k in range(n):
        u_turn[k, SW:, :] = ones
    w_tile[...] = jnp.broadcast_to(w_in[...], w_tile.shape)
    pl.semaphore_wait(barrier, n + head_shards - 2)

    direct = []
    for i in range(1, heads):
        h = flip(i)
        device = h * group + member
        direct += [
            remote(t_in.at[:, columns(h)], t_all.at[rows(me)], t_send.at[i], t_recv.at[me], device),
            remote(u_in.at[head_rows(h)], u_turn.at[me, pl.ds(0, SW)], u_send.at[i], u_recv.at[me], device),
            remote(w_tile, w_all.at[head], w_send.at[i], w_recv.at[head], device),
        ]
    for copy in direct:
        copy.start()

    def forwards(i, slot, t_src, u_src):
        return [
            remote(t_src, t_all.at[rows(slot)], t_fwd.at[i], t_recv.at[slot], mate),
            remote(u_src, u_turn.at[slot, pl.ds(0, SW)], u_fwd.at[i], u_recv.at[slot], mate),
        ]

    def arrived(slot):
        remote(t_in.at[:, columns(0)], t_all.at[rows(slot)], t_send.at[0], t_recv.at[slot], mate).wait_recv()
        remote(u_in.at[head_rows(0)], u_turn.at[slot, pl.ds(0, SW)], u_send.at[0], u_recv.at[slot], mate).wait_recv()

    for copy in forwards(0, me, t_in.at[:, columns(head)], u_in.at[head_rows(head)]):
        copy.start()
    own_t = pltpu.make_async_copy(t_in.at[:, columns(head)], t_all.at[rows(me)], own_sem.at[0])
    own_t.start()
    u_turn[me, :SW, :] = u_in[head_rows(head), :]
    w_all[head] = w_tile[...]
    lane = lax.broadcasted_iota(jnp.int32, (block, LANES), 1)

    def turn_u(slot):
        u_all[rows(slot), :] = jnp.where(lane < SW, u_turn[slot].astype(jnp.float32).T, 0.0).astype(jnp.bfloat16)

    for h in range(heads):
        t_top[h] = jnp.full((8, block), -1e30, jnp.float32)
        u_top[h] = jnp.full((8, block), -1e30, jnp.float32)
        cross[h] = jnp.zeros((8, block), jnp.float32)
        t_rows[h] = jnp.zeros((LANES, block), jnp.float32)
        u_rows[h] = jnp.zeros((LANES, block), jnp.float32)

    def fold(x, op):
        return op(x.reshape(x.shape[0] // 8, 8, block), axis=0)

    def unit(i, k):
        early = k < i
        return flip(jnp.where(early, i, k - i)), flip(jnp.where(early, k, i))

    def scores(i, k, b):
        own, key = unit(i, k)
        slot = own * group + member
        t = dot_nt(t_all[both_rows(key), :], t_all[rows(slot), :])
        u = jnp.dot(u_all[both_rows(key), :], u_turn[slot], preferred_element_type=jnp.float32)
        t_raw[b] = t
        u_raw[b] = u
        return fold(t, jnp.max), fold(u, jnp.max)

    def soften(i, k, b, peaks):
        own, key = unit(i, k)

        def side(raw_ref, peak, scale, top, refs, exps, out, with_cross):
            raw = raw_ref[b]
            old = top[own]
            new = jnp.maximum(old, jnp.max(peak, axis=0, keepdims=True))
            top[own] = new
            refs[own, pl.ds(key, 1), :] = new[:1] * scale
            value = jnp.exp2(raw * scale - new[:1] * scale).astype(jnp.bfloat16)
            keep = jnp.exp2((old - new) * scale)
            if with_cross:
                cross[own] = cross[own] * keep + fold(value.astype(jnp.float32) * raw, jnp.sum)
            total = out[own] * keep[:1]
            for q in range(group):
                piece = value[q * block:(q + 1) * block]
                exps[own, key * group + q] = piece
                total = total + jnp.dot(u_turn[key * group + q], piece, preferred_element_type=jnp.float32)
            out[own] = total

        side(t_raw, peaks[0], t_scale, t_top, t_refs, t_exp, t_rows, True)
        side(u_raw, peaks[1], u_scale, u_top, u_refs, u_exp, u_rows, False)

    turn_u(me)
    own_t.wait()
    arrived(head * group + 1 - member)
    turn_u(head * group + 1 - member)
    soften(0, 0, 0, scores(0, 0, 0))

    def arrival(i, carry):
        h = flip(i)
        slot = h * group + member
        other = h * group + 1 - member
        arrived(slot)
        for copy in forwards(i, slot, t_all.at[rows(slot)], u_turn.at[slot, pl.ds(0, SW)]):
            copy.start()
        turn_u(slot)

        def run(k, count, peaks):
            for z in range(count):
                ahead = scores(i, k + z + 1, (z + 1) % 2)
                soften(i, k + z, z % 2, peaks)
                peaks = ahead
            return peaks

        def whole():
            arrived(other)
            turn_u(other)

        def four(j, peaks):
            pl.when(j == lax.div(i - 1, 4))(whole)
            return run(4 * j, 4, peaks)

        def two(j, peaks):
            pl.when(i == 1)(whole)
            return run(2 * i - 2, 2, peaks)

        peaks = lax.fori_loop(0, lax.div(i, 2), four, scores(i, 0, 0))
        soften(i, 2 * i, 0, lax.fori_loop(0, lax.rem(i, 2), two, peaks))
        return carry

    lax.fori_loop(1, heads, arrival, 0)
    for i in range(1, heads):
        remote(w_tile, w_all.at[flip(i)], w_send.at[0], w_recv.at[flip(i)], mate).wait_recv()

    loss = jnp.zeros((1, block), jnp.float32)
    for h in range(heads):
        weight = w_all[h][:1, :]
        t_sum = t_rows[h, SW:SW + 1, :]
        u_sum = u_rows[h, SW:SW + 1, :]
        t_norm = t_top[h][:1] * t_scale + jnp.log(t_sum) * LOG2E
        u_norm = u_top[h][:1] * u_scale + jnp.log(u_sum) * LOG2E
        own_u = u_turn[h * group + member].astype(jnp.float32)[:SW]
        seen = jnp.sum(own_u * t_rows[h, :SW, :], axis=0, keepdims=True) * u_scale
        mean = (jnp.sum(cross[h], axis=0, keepdims=True) * t_scale - seen) / t_sum
        loss = loss + weight * (mean - t_norm + u_norm)
        t_part = weight / t_sum
        u_part = weight / u_sum
        t_last = t_top[h][:1] * t_scale
        u_last = u_top[h][:1] * u_scale
        t_refs[h] = jnp.exp2(t_refs[h] - t_last) * t_part
        u_refs[h] = jnp.exp2(u_refs[h] - u_last) * u_part
        u_rows[h] = u_rows[h] * u_part - t_rows[h] * t_part
    loss = jnp.sum(loss, axis=1, keepdims=True) * (LN2 / (heads * head_shards * block * n))
    losses[me] = jnp.broadcast_to(loss, losses.shape[1:])
    stats = [
        remote(losses.at[me], losses.at[me], l_send.at[i], l_recv.at[me], lax.rem(me + i, n))
        for i in range(1, n)
    ]
    for copy in stats:
        copy.start()

    def column_part(h, q):
        key = h * group + q
        total = jnp.zeros((LANES, block), jnp.float32)
        for own in range(heads):
            t_part = t_exp[own, key].astype(jnp.float32) * t_refs[own, pl.ds(h, 1), :]
            u_part = u_exp[own, key].astype(jnp.float32) * u_refs[own, pl.ds(h, 1), :]
            total = total + dot_nt(u_turn[own * group + member], (u_part - t_part).astype(jnp.bfloat16))
        return total[:SW]

    def swap(h):
        return remote(parts.at[h], landed_parts.at[h], p_send.at[h], p_recv.at[h], mate)

    def give(i, h):
        return remote(code_out.at[h], code_in.at[head], g_send.at[i], g_recv.at[head], h * group + member)

    def finish(h):
        swap(h).wait_recv()
        return (grads[h] + landed_parts[h]) * (1.0 / math.sqrt(SW))

    def encode(h):
        grad = finish(h)
        peak = jnp.maximum(jnp.max(jnp.abs(grad), axis=0, keepdims=True), 1e-30)
        peak = (peak * 1.01).astype(jnp.bfloat16)
        code_out[h, SW:, :] = jnp.broadcast_to(peak, (LANES - SW, block))
        code_out[h, :SW, :] = jnp.exp2(grad * (SPAN / peak.astype(jnp.float32))).astype(jnp.bfloat16)

    def hand_over(i):
        h = flip(i)
        encode(h)
        give(i, h).start()

    def step(j, carry):
        i = heads - 1 - j
        h = flip(i)
        parts[h] = column_part(h, 1 - member)
        swap(h).start()

        @pl.when(j > 0)
        def _():
            hand_over(i + 1)
        grads[h] = column_part(h, member) + u_rows[h, :SW, :]
        return carry

    lax.fori_loop(0, heads, step, 0)
    for i in range(1, n):
        peer = lax.rem(me + i, n)
        remote(losses.at[peer], losses.at[peer], l_send.at[0], l_recv.at[peer], mate).wait_recv()
    sums[shard] = jnp.sum(losses[...], axis=0)
    shards = [
        remote(sums.at[shard], sums.at[shard], s_send.at[i], s_recv.at[shard], {"head": lax.rem(shard + i, head_shards)})
        for i in range(1, head_shards)
    ]
    for copy in shards:
        copy.start()
    encode(head)
    own_code = pltpu.make_async_copy(code_out.at[head], code_in.at[head], own_sem.at[1])
    own_code.start()
    for i in range(1, head_shards):
        peer = lax.rem(shard + i, head_shards)
        remote(sums.at[peer], sums.at[peer], s_send.at[0], s_recv.at[peer], {"head": peer}).wait_recv()
    loss_out[0, 0] = jnp.max(jnp.sum(sums[...], axis=0))

    for copy in direct + stats + shards:
        copy.wait_send()
    for i in range(heads):
        for copy in forwards(i, me, t_in.at[:, columns(0)], u_in.at[head_rows(0)]):
            copy.wait_send()
        swap(flip(i)).wait_send()
    for i in range(1, heads):
        give(i, flip(i)).wait_send()
    own_code.wait()
    for i in range(1, heads):
        h = flip(i)
        remote(code_out.at[h], code_in.at[h], g_send.at[0], g_recv.at[h], mate).wait_recv()

def decode_kernel(heads, codes, loss_in, grad_out, loss_out, flat, tall, sem):
    loss_out[0, 0] = loss_in[0, 0]
    chunks = heads * SW // LANES

    def write(c):
        columns = pl.ds(c * LANES, LANES)
        return pltpu.make_async_copy(tall.at[:, columns], grad_out.at[:, columns], sem.at[c])

    ready = 0
    for h in range(heads):
        code = codes[h].astype(jnp.float32)
        flat[h * SW:(h + 1) * SW, :] = jnp.log(code[:SW]) * (code[SW:SW + 1] * (LOG2E / SPAN))
        while (ready + 1) * LANES <= (h + 1) * SW:
            tall[:, ready * LANES:(ready + 1) * LANES] = flat[ready * LANES:(ready + 1) * LANES, :].T
            write(ready).start()
            ready += 1
    for c in range(chunks):
        write(c).wait()


def decode_call(heads, block):
    smem = pl.BlockSpec(memory_space=pltpu.SMEM)
    return pl.pallas_call(
        functools.partial(decode_kernel, heads),
        out_shape=(
            jax.ShapeDtypeStruct((block, heads * SW), jnp.float32),
            jax.ShapeDtypeStruct((1, 1), jnp.float32),
        ),
        in_specs=[pl.BlockSpec(memory_space=pltpu.VMEM), smem],
        out_specs=(pl.BlockSpec(memory_space=pl.ANY), smem),
        scratch_shapes=[
            pltpu.VMEM((heads * SW, block), jnp.float32),
            pltpu.VMEM((block, heads * SW), jnp.float32),
            pltpu.SemaphoreType.DMA((heads * SW // LANES,)),
        ],
    )


def pair_call(heads, n, head_shards, block):
    vmem = pl.BlockSpec(memory_space=pltpu.VMEM)
    dma = pltpu.SemaphoreType.DMA
    f32, bf16 = jnp.float32, jnp.bfloat16
    return pl.pallas_call(
        functools.partial(pair_kernel, heads, head_shards),
        out_shape=(
            jax.ShapeDtypeStruct((heads, LANES, block), bf16),
            jax.ShapeDtypeStruct((1, 1), f32),
        ),
        in_specs=[pl.BlockSpec(memory_space=pl.ANY), vmem, vmem],
        out_specs=(pl.BlockSpec(memory_space=pl.ANY), pl.BlockSpec(memory_space=pltpu.SMEM)),
        scratch_shapes=[
            pltpu.VMEM((heads * SW, block), bf16),
            pltpu.VMEM((8, block), f32),
            pltpu.VMEM((n * block, TW), bf16),
            pltpu.VMEM((n * block, LANES), bf16),
            pltpu.VMEM((n, LANES, block), bf16),
            pltpu.VMEM((heads, 8, block), f32),
            pltpu.VMEM((2, 2 * block, block), f32),
            pltpu.VMEM((2, 2 * block, block), f32),
            pltpu.VMEM((heads, n, block, block), bf16),
            pltpu.VMEM((heads, n, block, block), bf16),
            pltpu.VMEM((heads, heads, block), f32),
            pltpu.VMEM((heads, heads, block), f32),
            pltpu.VMEM((heads, 8, block), f32),
            pltpu.VMEM((heads, 8, block), f32),
            pltpu.VMEM((heads, 8, block), f32),
            pltpu.VMEM((heads, LANES, block), f32),
            pltpu.VMEM((heads, LANES, block), f32),
            pltpu.VMEM((heads, SW, block), f32),
            pltpu.VMEM((heads, SW, block), f32),
            pltpu.VMEM((heads, SW, block), f32),
            pltpu.VMEM((heads, LANES, block), bf16),
            pltpu.VMEM((n, 8, LANES), f32),
            pltpu.VMEM((head_shards, 8, LANES), f32),
            dma((heads,)), dma((heads,)), dma((heads,)),
            dma((heads,)), dma((heads,)),
            dma((n,)), dma((n,)), dma((heads,)),
            dma((heads,)), dma((heads,)),
            dma((heads,)), dma((heads,)),
            dma((n,)), dma((n,)), dma((head_shards,)), dma((head_shards,)), dma((2,)),
        ],
        compiler_params=pltpu.CompilerParams(
            collective_id=1, has_side_effects=True, vmem_limit_bytes=60 * 2**20
        ),
    )


def local(teacher, student, weights):
    relations, block, t_columns = teacher.shape
    assert relations == 1
    heads = t_columns // TW
    n = lax.axis_size("seq")
    head_shards = lax.axis_size("head")
    assert n % heads == 0
    group = n // heads
    if group == 2 and heads & (heads - 1) == 0 and heads * SW % LANES == 0 and n * n * block * block <= 2**24:
        codes, loss = pair_call(heads, n, head_shards, block)(teacher[0], student[0], weights[None, :])
        student_grad, loss = decode_call(heads, block)(codes, loss)
        return (loss.reshape(()), student_grad[None])
    vmem = pl.BlockSpec(memory_space=pltpu.VMEM)
    dma = pltpu.SemaphoreType.DMA
    student_grad, loss = pl.pallas_call(
        functools.partial(kernel, heads, group, head_shards),
        out_shape=(
            jax.ShapeDtypeStruct((block, heads * SW), jnp.float32),
            jax.ShapeDtypeStruct((8, LANES), jnp.float32),
        ),
        in_specs=[vmem] * 3,
        out_specs=(vmem, vmem),
        scratch_shapes=[
            pltpu.VMEM((heads, block, LANES), jnp.bfloat16),
            pltpu.VMEM((8, block), jnp.float32),
            pltpu.VMEM((n * block, TW), jnp.bfloat16),
            pltpu.VMEM((n * block, LANES), jnp.bfloat16),
            pltpu.VMEM((heads, 8, block), jnp.float32),
            pltpu.VMEM((heads, 5, 8, block), jnp.float32),
            pltpu.VMEM((group, heads, 16, block), jnp.float32),
            pltpu.VMEM((heads, block, LANES), jnp.float32),
            pltpu.VMEM((heads, block, LANES), jnp.float32),
            pltpu.VMEM((n, 8, LANES), jnp.float32),
            pltpu.VMEM((head_shards, 8, LANES), jnp.float32),
            dma((heads,)), dma((heads,)), dma((heads,)),
            dma((heads, group)), dma((heads, group)),
            dma((n,)), dma((n,)), dma((heads,)),
            dma((group,)), dma((group,)),
            dma((heads,)), dma((heads,)),
            dma((n,)), dma((n,)), dma((head_shards,)), dma((head_shards,)),
        ],
        compiler_params=pltpu.CompilerParams(
            collective_id=0, has_side_effects=True, vmem_limit_bytes=60 * 2**20
        ),
    )(teacher[0], student[0], weights[None, :])
    return (loss[0, 0], student_grad[None])


def solution(mesh):
    return jax.shard_map(
        local,
        mesh=mesh,
        in_specs=(P(None, "seq", "head"), P(None, "seq", "head"), P("seq")),
        out_specs=(P(), P(None, "seq", "head")),
        check_vma=False,
    )
```

```python
import functools
import math

import jax
import jax.numpy as jnp
from jax import lax
from jax.experimental import pallas as pl
from jax.experimental.pallas import tpu as pltpu
from jax.sharding import PartitionSpec as P

TW = 256
SW = 112
LANES = 128
SPAN = 119.0
LOG2E = math.log2(math.e)
LN2 = math.log(2.0)
NT = (((1,), (1,)), ((), ()))


def dot_nt(a, b):
    return lax.dot_general(a, b, NT, preferred_element_type=jnp.float32)


def kernel(
    heads, group, head_shards, t_in, s_in, w_in, grad_out, loss_out,
    u_in, w_tile, t_all, u_all, w_all, state, norms, grads, landed, losses, sums,
    t_send, u_send, w_send, t_fwd, u_fwd, t_recv, u_recv, w_recv, n_send, n_recv, g_send, g_recv,
    l_send, l_recv, s_send, s_recv,
):
    n = heads * group
    block = t_in.shape[0]
    me = lax.axis_index("seq")
    shard = lax.axis_index("head")
    head = lax.div(me, group)
    member = lax.rem(me, group)
    unroll = math.gcd(n, 8)
    pair = math.gcd(heads, 2)
    t_scale = LOG2E / math.sqrt(TW)
    u_scale = LOG2E / math.sqrt(SW)

    def other_head(i):
        return lax.rem(head + i, heads)

    def source_head(i):
        return lax.rem(head + heads - i, heads)

    def other_member(i):
        return lax.rem(member + i, group)

    def remote(src, dst, send, recv, device):
        target = device if isinstance(device, dict) else {"seq": device}
        return pltpu.make_async_remote_copy(
            src_ref=src, dst_ref=dst, send_sem=send, recv_sem=recv,
            device_id=target, device_id_type=pl.DeviceIdType.MESH,
        )

    def rows(slot):
        return pl.ds(pl.multiple_of(slot * block, block), block)

    def columns(h):
        return pl.ds(pl.multiple_of(h * TW, TW), TW)

    barrier = pltpu.get_barrier_semaphore()
    for i in range(1, n):
        pl.semaphore_signal(barrier, inc=1, device_id={"seq": lax.rem(me + i, n)}, device_id_type=pl.DeviceIdType.MESH)
    for i in range(1, head_shards):
        pl.semaphore_signal(barrier, inc=1, device_id={"head": lax.rem(shard + i, head_shards)}, device_id_type=pl.DeviceIdType.MESH)
    for h in range(heads):
        u_in[h] = jnp.concatenate(
            [s_in[:, h * SW:(h + 1) * SW], jnp.zeros((block, LANES - SW), jnp.bfloat16)], axis=1
        )
    w_tile[...] = jnp.broadcast_to(w_in[...], w_tile.shape)
    pl.semaphore_wait(barrier, n + head_shards - 2)

    direct = []
    for i in range(1, heads):
        h = other_head(i)
        device = h * group + member
        direct += [
            remote(t_in.at[:, columns(h)], t_all.at[rows(me)], t_send.at[i], t_recv.at[me], device),
            remote(u_in.at[h], u_all.at[rows(me)], u_send.at[i], u_recv.at[me], device),
            remote(w_tile, w_all.at[head], w_send.at[i], w_recv.at[head], device),
        ]
    for copy in direct:
        copy.start()

    def forwards(i, slot, t_src, u_src):
        pairs = []
        for g in range(1, group):
            device = head * group + other_member(g)
            pairs += [
                remote(t_src, t_all.at[rows(slot)], t_fwd.at[i, g], t_recv.at[slot], device),
                remote(u_src, u_all.at[rows(slot)], u_fwd.at[i, g], u_recv.at[slot], device),
            ]
        return pairs

    def arrived(slot):
        remote(t_in.at[:, columns(0)], t_all.at[rows(slot)], t_send.at[0], t_recv.at[slot], me).wait_recv()
        remote(u_in.at[0], u_all.at[rows(slot)], u_send.at[0], u_recv.at[slot], me).wait_recv()

    for copy in forwards(0, me, t_in.at[:, columns(head)], u_in.at[head]):
        copy.start()
    t_all[rows(me), :] = t_in[:, columns(head)]
    u_all[rows(me), :] = u_in[head]
    w_all[head] = w_tile[...]

    low = jnp.full((8, block), -1e30, jnp.float32)
    zero = jnp.zeros((8, block), jnp.float32)
    for h in range(heads):
        for k, value in enumerate((low, zero, zero, low, zero)):
            state[h, k] = value

    def tile(row_head, key_pair):
        t_own = t_all[rows(row_head * group + member), :]
        u_own = u_all[rows(row_head * group + member), :]
        width = math.gcd(group, 2)
        parts = [(a, q) for a in range(pair) for q in range(width)]

        def step(j, carry):
            t_max, t_sum, t_cross, u_max, u_sum = carry
            for a, q in parts:
                keys = rows(source_head(key_pair * pair + a) * group + j * width + q)
                t_score = (dot_nt(t_all[keys, :], t_own) * t_scale).reshape(block // 8, 8, block)
                u_score = (dot_nt(u_all[keys, :], u_own) * u_scale).reshape(block // 8, 8, block)
                t_top = jnp.maximum(t_max, jnp.max(t_score, axis=0))
                u_top = jnp.maximum(u_max, jnp.max(u_score, axis=0))
                t_exp = jnp.exp2(t_score - t_top[None])
                u_exp = jnp.exp2(u_score - u_top[None])
                t_keep = jnp.exp2(t_max - t_top)
                u_keep = jnp.exp2(u_max - u_top)
                t_sum = t_sum * t_keep + jnp.sum(t_exp, axis=0)
                t_cross = t_cross * t_keep + jnp.sum(t_exp * (t_score - u_score), axis=0)
                u_sum = u_sum * u_keep + jnp.sum(u_exp, axis=0)
                t_max, u_max = t_top, u_top
            return t_max, t_sum, t_cross, u_max, u_sum

        carry = tuple(state[row_head, k] for k in range(5))
        carry = step(0, carry) if group == width else lax.fori_loop(0, group // width, step, carry)
        for k in range(5):
            state[row_head, k] = carry[k]

    def arrival(p, carry):
        for a in range(pair):
            i = p * pair + a
            h = source_head(i)
            slot = h * group + member

            @pl.when(i > 0)
            def _(i=i, slot=slot):
                arrived(slot)
                for copy in forwards(i, slot, t_all.at[rows(slot)], u_all.at[rows(slot)]):
                    copy.start()
        for a in range(pair):
            h = source_head(p * pair + a)
            for g in range(1, group):
                arrived(h * group + other_member(g))

        def one(j, carry):
            old = j < p * pair
            fresh = j - p * pair
            tile(
                source_head(jnp.where(old, j, p * pair + lax.rem(fresh, pair))),
                jnp.where(old, p, lax.div(fresh, pair)),
            )
            return carry

        return lax.fori_loop(0, p * pair + (p + 1) * pair, one, carry)

    lax.fori_loop(0, heads // pair, arrival, 0)
    for i in range(1, heads):
        remote(w_tile, w_all.at[source_head(i)], w_send.at[0], w_recv.at[source_head(i)], me).wait_recv()

    loss = jnp.zeros((1, block), jnp.float32)
    for i in range(heads):
        t_max, t_sum, t_cross, u_max, u_sum = (state[i, k] for k in range(5))
        t_top = jnp.max(t_max, axis=0, keepdims=True)
        u_top = jnp.max(u_max, axis=0, keepdims=True)
        t_keep = jnp.exp2(t_max - t_top)
        t_total = jnp.sum(t_sum * t_keep, axis=0, keepdims=True)
        t_mixed = jnp.sum(t_cross * t_keep, axis=0, keepdims=True)
        u_total = jnp.sum(u_sum * jnp.exp2(u_max - u_top), axis=0, keepdims=True)
        t_norm = t_top + jnp.log(t_total) * LOG2E
        u_norm = u_top + jnp.log(u_total) * LOG2E
        weight = w_all[i][:1, :]
        weight_log = jnp.log(weight) * LOG2E
        norms[member, i, 0:8, :] = jnp.broadcast_to(t_norm - weight_log, (8, block))
        norms[member, i, 8:16, :] = jnp.broadcast_to(u_norm - weight_log, (8, block))
        loss = loss + weight * (t_mixed / t_total - t_norm + u_norm)
    loss = jnp.sum(loss, axis=1, keepdims=True) * (LN2 / (heads * head_shards * block * n))
    losses[me] = jnp.broadcast_to(loss, losses.shape[1:])
    stats = [
        remote(norms.at[member], norms.at[member], n_send.at[g], n_recv.at[member], head * group + other_member(g))
        for g in range(1, group)
    ]
    for i in range(1, n):
        stats.append(remote(losses.at[me], losses.at[me], l_send.at[i], l_recv.at[me], lax.rem(me + i, n)))
    for copy in stats:
        copy.start()
    for g in range(1, group):
        m = other_member(g)
        remote(norms.at[m], norms.at[m], n_send.at[0], n_recv.at[m], me).wait_recv()

    def row_grad(i):
        slot = i * group + member
        t_own = t_all[rows(slot), :]
        u_own = u_all[rows(slot), :]

        def own_norm(first):
            tall = jnp.broadcast_to(norms[member, i, first:first + 1, :], (LANES, block)).T
            return jnp.concatenate([tall] * (block // LANES), axis=1)

        t_mine = own_norm(0)
        u_mine = own_norm(8)

        def step(j, total):
            for q in range(unroll):
                key = j * unroll + q
                keys = rows(key)
                key_head = lax.div(key, group)
                key_member = lax.rem(key, group)
                t_theirs = norms[key_member, key_head, 0:1, :]
                u_theirs = norms[key_member, key_head, 8:9, :]
                u_keys = u_all[keys, :]
                t_score = dot_nt(t_own, t_all[keys, :]) * t_scale
                u_score = dot_nt(u_own, u_keys) * u_scale
                row_part = jnp.exp2(u_score - u_mine) - jnp.exp2(t_score - t_mine)
                col_part = jnp.exp2(u_score - u_theirs) - jnp.exp2(t_score - t_theirs)
                mix = (row_part + col_part).astype(jnp.bfloat16)
                total = total + jnp.dot(mix, u_keys, preferred_element_type=jnp.float32)
            return total

        total = lax.fori_loop(0, n // unroll, step, jnp.zeros((block, LANES), jnp.float32))
        return total * (1.0 / math.sqrt(SW))

    def send_grad(i, h):
        return remote(grads.at[h], landed.at[head], g_send.at[h], g_recv.at[head], h * group + member)

    def grad_step(i, carry):
        h = other_head(i)
        grads[h] = row_grad(h)
        send_grad(i, h).start()
        return carry

    lax.fori_loop(1, heads, grad_step, 0)
    for i in range(1, n):
        peer = lax.rem(me + i, n)
        remote(losses.at[peer], losses.at[peer], l_send.at[0], l_recv.at[peer], me).wait_recv()
    sums[shard] = jnp.sum(losses[...], axis=0)
    shards = [
        remote(sums.at[shard], sums.at[shard], s_send.at[i], s_recv.at[shard], {"head": lax.rem(shard + i, head_shards)})
        for i in range(1, head_shards)
    ]
    for copy in shards:
        copy.start()
    landed[head] = row_grad(head)
    for i in range(1, head_shards):
        peer = lax.rem(shard + i, head_shards)
        remote(sums.at[peer], sums.at[peer], s_send.at[0], s_recv.at[peer], {"head": peer}).wait_recv()
    loss_out[...] = jnp.sum(sums[...], axis=0)

    for copy in direct + stats + shards:
        copy.wait_send()
    for i in range(heads):
        for copy in forwards(i, me, t_in.at[:, columns(0)], u_in.at[0]):
            copy.wait_send()
    for i in range(1, heads):
        send_grad(i, other_head(i)).wait_send()
    for h in range(heads):
        @pl.when(head != h)
        def _(h=h):
            remote(grads.at[h], landed.at[h], g_send.at[h], g_recv.at[h], me).wait_recv()
        grad_out[:, h * SW:(h + 1) * SW] = landed[h][:, :SW]


def pair_kernel(
    heads, head_shards, t_in, s_in, w_in, code_in, peak_in, loss_out,
    u_in, w_tile, t_all, u_all, u_turn, w_all, t_raw, u_raw, t_exp, u_exp, t_refs, u_refs, t_top, u_top, cross,
    t_rows, u_rows, parts, landed_parts, code_out, peak_out, losses, sums,
    t_send, u_send, w_send, t_fwd, u_fwd, t_recv, u_recv, w_recv, p_send, p_recv, g_send, g_recv,
    l_send, l_recv, s_send, s_recv, own_sem, k_send, k_recv,
):
    group = 2
    n = heads * group
    block = t_in.shape[0]
    both = group * block
    me = lax.axis_index("seq")
    shard = lax.axis_index("head")
    head = lax.div(me, group)
    member = lax.rem(me, group)
    mate = head * group + 1 - member
    bits = (heads - 1).bit_length()
    t_scale = LOG2E / math.sqrt(TW)
    u_scale = LOG2E / math.sqrt(SW)

    half = heads // 2
    quarter = max(heads // 4, 1)

    def flip(i):
        i = jnp.int32(i)
        if heads >= 4:
            turned = half + lax.rem(i - half, 2) * quarter + lax.div(i - half, 2)
            i = i + lax.div(i, half) * (turned - i)
        out = 0
        for k in range(bits):
            out = out + lax.rem(lax.div(head, 2**k) + lax.div(jnp.int32(i), 2**k), 2) * 2**k
        return out

    def remote(src, dst, send, recv, device):
        target = device if isinstance(device, dict) else {"seq": device}
        return pltpu.make_async_remote_copy(
            src_ref=src, dst_ref=dst, send_sem=send, recv_sem=recv,
            device_id=target, device_id_type=pl.DeviceIdType.MESH,
        )

    def rows(slot):
        return pl.ds(pl.multiple_of(slot * block, block), block)

    def both_rows(h):
        return pl.ds(pl.multiple_of(h * both, both), both)

    def head_rows(h):
        return pl.ds(pl.multiple_of(h * SW, 16), SW)

    def columns(h):
        return pl.ds(pl.multiple_of(h * TW, TW), TW)

    barrier = pltpu.get_barrier_semaphore()
    for i in range(1, n):
        pl.semaphore_signal(barrier, inc=1, device_id={"seq": lax.rem(me + i, n)}, device_id_type=pl.DeviceIdType.MESH)
    for i in range(1, head_shards):
        pl.semaphore_signal(barrier, inc=1, device_id={"head": lax.rem(shard + i, head_shards)}, device_id_type=pl.DeviceIdType.MESH)
    for c in range(heads * SW // LANES):
        piece = s_in[:, c * LANES:(c + 1) * LANES].astype(jnp.float32)
        u_in[c * LANES:(c + 1) * LANES, :] = piece.T.astype(jnp.bfloat16)
    spare = lax.broadcasted_iota(jnp.int32, (LANES - SW, block), 0)
    ones = jnp.where(spare == 0, 1.0, 0.0).astype(jnp.bfloat16)
    for k in range(n):
        u_turn[k, SW:, :] = ones
    w_tile[...] = jnp.broadcast_to(w_in[...], w_tile.shape)
    pl.semaphore_wait(barrier, n + head_shards - 2)

    direct = []
    for i in range(1, heads):
        h = flip(i)
        device = h * group + member
        direct += [
            remote(t_in.at[:, columns(h)], t_all.at[rows(me)], t_send.at[i], t_recv.at[me], device),
            remote(u_in.at[head_rows(h)], u_turn.at[me, pl.ds(0, SW)], u_send.at[i], u_recv.at[me], device),
            remote(w_tile, w_all.at[head], w_send.at[i], w_recv.at[head], device),
        ]
    for copy in direct:
        copy.start()

    def forwards(i, slot, t_src, u_src):
        return [
            remote(t_src, t_all.at[rows(slot)], t_fwd.at[i], t_recv.at[slot], mate),
            remote(u_src, u_turn.at[slot, pl.ds(0, SW)], u_fwd.at[i], u_recv.at[slot], mate),
        ]

    def arrived(slot):
        remote(t_in.at[:, columns(0)], t_all.at[rows(slot)], t_send.at[0], t_recv.at[slot], mate).wait_recv()
        remote(u_in.at[head_rows(0)], u_turn.at[slot, pl.ds(0, SW)], u_send.at[0], u_recv.at[slot], mate).wait_recv()

    for copy in forwards(0, me, t_in.at[:, columns(head)], u_in.at[head_rows(head)]):
        copy.start()
    own_t = pltpu.make_async_copy(t_in.at[:, columns(head)], t_all.at[rows(me)], own_sem.at[0])
    own_t.start()
    u_turn[me, :SW, :] = u_in[head_rows(head), :]
    w_all[head] = w_tile[...]
    lane = lax.broadcasted_iota(jnp.int32, (block, LANES), 1)

    def turn_u(slot):
        u_all[rows(slot), :] = jnp.where(lane < SW, u_turn[slot].astype(jnp.float32).T, 0.0).astype(jnp.bfloat16)

    for h in range(heads):
        t_top[h] = jnp.full((8, block), -1e30, jnp.float32)
        u_top[h] = jnp.full((8, block), -1e30, jnp.float32)
        cross[h] = jnp.zeros((8, block), jnp.float32)
        t_rows[h] = jnp.zeros((LANES, block), jnp.float32)
        u_rows[h] = jnp.zeros((LANES, block), jnp.float32)

    def fold(x, op):
        return op(x.reshape(x.shape[0] // 8, 8, block), axis=0)

    def unit(i, k):
        early = k < i
        return flip(jnp.where(early, i, k - i)), flip(jnp.where(early, k, i))

    def scores(i, k, b):
        own, key = unit(i, k)
        slot = own * group + member
        t = dot_nt(t_all[both_rows(key), :], t_all[rows(slot), :])
        u = jnp.dot(u_all[both_rows(key), :], u_turn[slot], preferred_element_type=jnp.float32)
        t_raw[b] = t
        u_raw[b] = u
        return fold(t, jnp.max), fold(u, jnp.max)

    def soften(i, k, b, peaks):
        own, key = unit(i, k)

        def side(raw_ref, peak, scale, top, refs, exps, out, with_cross):
            raw = raw_ref[b]
            old = top[own]
            new = jnp.maximum(old, jnp.max(peak, axis=0, keepdims=True))
            top[own] = new
            refs[own, pl.ds(key, 1), :] = new[:1] * scale
            value = jnp.exp2(raw * scale - new[:1] * scale).astype(jnp.bfloat16)
            keep = jnp.exp2((old - new) * scale)
            if with_cross:
                cross[own] = cross[own] * keep + fold(value.astype(jnp.float32) * raw, jnp.sum)
            total = out[own] * keep[:1]
            for q in range(group):
                piece = value[q * block:(q + 1) * block]
                exps[own, key * group + q] = piece
                total = total + jnp.dot(u_turn[key * group + q], piece, preferred_element_type=jnp.float32)
            out[own] = total

        side(t_raw, peaks[0], t_scale, t_top, t_refs, t_exp, t_rows, True)
        side(u_raw, peaks[1], u_scale, u_top, u_refs, u_exp, u_rows, False)

    turn_u(me)
    own_t.wait()
    arrived(head * group + 1 - member)
    turn_u(head * group + 1 - member)
    soften(0, 0, 0, scores(0, 0, 0))

    def arrival(i, carry):
        h = flip(i)
        slot = h * group + member
        other = h * group + 1 - member
        arrived(slot)
        for copy in forwards(i, slot, t_all.at[rows(slot)], u_turn.at[slot, pl.ds(0, SW)]):
            copy.start()
        turn_u(slot)

        def run(k, count, peaks):
            for z in range(count):
                ahead = scores(i, k + z + 1, (z + 1) % 2)
                soften(i, k + z, z % 2, peaks)
                peaks = ahead
            return peaks

        def whole():
            arrived(other)
            turn_u(other)

        def four(j, peaks):
            pl.when(j == lax.div(i - 1, 4))(whole)
            return run(4 * j, 4, peaks)

        def two(j, peaks):
            pl.when(i == 1)(whole)
            return run(2 * i - 2, 2, peaks)

        peaks = lax.fori_loop(0, lax.div(i, 2), four, scores(i, 0, 0))
        soften(i, 2 * i, 0, lax.fori_loop(0, lax.rem(i, 2), two, peaks))
        return carry

    lax.fori_loop(1, heads, arrival, 0)
    for i in range(1, heads):
        remote(w_tile, w_all.at[flip(i)], w_send.at[0], w_recv.at[flip(i)], mate).wait_recv()

    loss = jnp.zeros((1, block), jnp.float32)
    for h in range(heads):
        weight = w_all[h][:1, :]
        t_sum = t_rows[h, SW:SW + 1, :]
        u_sum = u_rows[h, SW:SW + 1, :]
        t_norm = t_top[h][:1] * t_scale + jnp.log(t_sum) * LOG2E
        u_norm = u_top[h][:1] * u_scale + jnp.log(u_sum) * LOG2E
        own_u = u_turn[h * group + member].astype(jnp.float32)[:SW]
        seen = jnp.sum(own_u * t_rows[h, :SW, :], axis=0, keepdims=True) * u_scale
        mean = (jnp.sum(cross[h], axis=0, keepdims=True) * t_scale - seen) / t_sum
        loss = loss + weight * (mean - t_norm + u_norm)
        t_part = weight / t_sum
        u_part = weight / u_sum
        t_last = t_top[h][:1] * t_scale
        u_last = u_top[h][:1] * u_scale
        t_refs[h] = jnp.exp2(t_refs[h] - t_last) * t_part
        u_refs[h] = jnp.exp2(u_refs[h] - u_last) * u_part
        u_rows[h] = u_rows[h] * u_part - t_rows[h] * t_part
    loss = jnp.sum(loss, axis=1, keepdims=True) * (LN2 / (heads * head_shards * block * n))
    losses[me] = jnp.broadcast_to(loss, losses.shape[1:])
    stats = [
        remote(losses.at[me], losses.at[me], l_send.at[i], l_recv.at[me], lax.rem(me + i, n))
        for i in range(1, n)
    ]
    for copy in stats:
        copy.start()

    def column_parts(h):
        total = jnp.zeros((both, LANES), jnp.float32)
        for own in range(heads):
            t_part = t_exp[own, pl.ds(h * group, group)].astype(jnp.float32) * t_refs[own, pl.ds(h, 1), :]
            u_part = u_exp[own, pl.ds(h * group, group)].astype(jnp.float32) * u_refs[own, pl.ds(h, 1), :]
            mix = (u_part - t_part).astype(jnp.bfloat16).reshape(both, block)
            total = total + jnp.dot(
                mix, u_all[rows(own * group + member), :], preferred_element_type=jnp.float32
            )
        for q in range(group):
            parts[h, q] = total[q * block:(q + 1) * block].T[:SW]

    def swap(h):
        return remote(parts.at[h, 1 - member], landed_parts.at[h], p_send.at[h], p_recv.at[h], mate)

    def give(i, h):
        return remote(code_out.at[h], code_in.at[head], g_send.at[i], g_recv.at[head], h * group + member)

    def give_peak(i, h):
        return remote(peak_out.at[h], peak_in.at[head], k_send.at[i], k_recv.at[head], h * group + member)

    def finish(h):
        swap(h).wait_recv()
        return (parts[h, member] + u_rows[h, :SW, :] + landed_parts[h]) * (1.0 / math.sqrt(SW))

    def encode(h):
        grad = finish(h)
        peak = jnp.maximum(jnp.max(jnp.abs(grad), axis=0, keepdims=True), 1e-30)
        code_out[h] = jnp.exp2(grad * (SPAN / peak)).astype(jnp.bfloat16)
        peak_out[h] = peak

    def hand_over(i):
        h = flip(i)
        encode(h)
        give(i, h).start()
        give_peak(i, h).start()

    def step(j, carry):
        i = heads - 1 - j
        h = flip(i)
        column_parts(h)
        swap(h).start()

        @pl.when(j > 0)
        def _():
            hand_over(i + 1)
        return carry

    lax.fori_loop(0, heads, step, 0)
    for i in range(1, n):
        peer = lax.rem(me + i, n)
        remote(losses.at[peer], losses.at[peer], l_send.at[0], l_recv.at[peer], mate).wait_recv()
    sums[shard] = jnp.sum(losses[...], axis=0)
    shards = [
        remote(sums.at[shard], sums.at[shard], s_send.at[i], s_recv.at[shard], {"head": lax.rem(shard + i, head_shards)})
        for i in range(1, head_shards)
    ]
    for copy in shards:
        copy.start()
    encode(head)
    own_code = pltpu.make_async_copy(code_out.at[head], code_in.at[head], own_sem.at[1])
    own_code.start()
    own_peak = pltpu.make_async_copy(peak_out.at[head], peak_in.at[head], own_sem.at[2])
    own_peak.start()
    for i in range(1, head_shards):
        peer = lax.rem(shard + i, head_shards)
        remote(sums.at[peer], sums.at[peer], s_send.at[0], s_recv.at[peer], {"head": peer}).wait_recv()
    loss_out[0, 0] = jnp.max(jnp.sum(sums[...], axis=0))

    for copy in direct + stats + shards:
        copy.wait_send()
    for i in range(heads):
        for copy in forwards(i, me, t_in.at[:, columns(0)], u_in.at[head_rows(0)]):
            copy.wait_send()
        swap(flip(i)).wait_send()
    for i in range(1, heads):
        give(i, flip(i)).wait_send()
        give_peak(i, flip(i)).wait_send()
    own_code.wait()
    own_peak.wait()
    for i in range(1, heads):
        h = flip(i)
        remote(code_out.at[h], code_in.at[h], g_send.at[0], g_recv.at[h], mate).wait_recv()
        remote(peak_out.at[h], peak_in.at[h], k_send.at[0], k_recv.at[h], mate).wait_recv()

def decode_kernel(heads, codes, peaks, loss_in, grad_out, loss_out, flat):
    loss_out[0, 0] = loss_in[0, 0]
    ready = 0
    for h in range(heads):
        code = codes[h].astype(jnp.float32)
        flat[h * SW:(h + 1) * SW, :] = jnp.log(code) * (peaks[h] * (LOG2E / SPAN))
        while (ready + 1) * LANES <= (h + 1) * SW:
            columns = slice(ready * LANES, (ready + 1) * LANES)
            grad_out[:, columns] = flat[columns, :].T
            ready += 1


def decode_call(heads, block):
    smem = pl.BlockSpec(memory_space=pltpu.SMEM)
    return pl.pallas_call(
        functools.partial(decode_kernel, heads),
        grid=(block // LANES,),
        out_shape=(
            jax.ShapeDtypeStruct((block, heads * SW), jnp.float32),
            jax.ShapeDtypeStruct((1, 1), jnp.float32),
        ),
        in_specs=[
            pl.BlockSpec((heads, SW, LANES), lambda i: (0, 0, i)),
            pl.BlockSpec((heads, 1, LANES), lambda i: (0, 0, i)),
            smem,
        ],
        out_specs=(pl.BlockSpec((LANES, heads * SW), lambda i: (i, 0)), smem),
        scratch_shapes=[pltpu.VMEM((heads * SW, LANES), jnp.float32)],
    )


def pair_call(heads, n, head_shards, block):
    vmem = pl.BlockSpec(memory_space=pltpu.VMEM)
    dma = pltpu.SemaphoreType.DMA
    f32, bf16 = jnp.float32, jnp.bfloat16
    return pl.pallas_call(
        functools.partial(pair_kernel, heads, head_shards),
        out_shape=(
            jax.ShapeDtypeStruct((heads, SW, block), bf16),
            jax.ShapeDtypeStruct((heads, 1, block), f32),
            jax.ShapeDtypeStruct((1, 1), f32),
        ),
        in_specs=[pl.BlockSpec(memory_space=pl.ANY), vmem, vmem],
        out_specs=(
            pl.BlockSpec(memory_space=pl.ANY), pl.BlockSpec(memory_space=pl.ANY), pl.BlockSpec(memory_space=pltpu.SMEM)
        ),
        scratch_shapes=[
            pltpu.VMEM((heads * SW, block), bf16),
            pltpu.VMEM((8, block), f32),
            pltpu.VMEM((n * block, TW), bf16),
            pltpu.VMEM((n * block, LANES), bf16),
            pltpu.VMEM((n, LANES, block), bf16),
            pltpu.VMEM((heads, 8, block), f32),
            pltpu.VMEM((2, 2 * block, block), f32),
            pltpu.VMEM((2, 2 * block, block), f32),
            pltpu.VMEM((heads, n, block, block), bf16),
            pltpu.VMEM((heads, n, block, block), bf16),
            pltpu.VMEM((heads, heads, block), f32),
            pltpu.VMEM((heads, heads, block), f32),
            pltpu.VMEM((heads, 8, block), f32),
            pltpu.VMEM((heads, 8, block), f32),
            pltpu.VMEM((heads, 8, block), f32),
            pltpu.VMEM((heads, LANES, block), f32),
            pltpu.VMEM((heads, LANES, block), f32),
            pltpu.VMEM((heads, 2, SW, block), f32),
            pltpu.VMEM((heads, SW, block), f32),
            pltpu.VMEM((heads, SW, block), bf16),
            pltpu.VMEM((heads, 1, block), f32),
            pltpu.VMEM((n, 8, LANES), f32),
            pltpu.VMEM((head_shards, 8, LANES), f32),
            dma((heads,)), dma((heads,)), dma((heads,)),
            dma((heads,)), dma((heads,)),
            dma((n,)), dma((n,)), dma((heads,)),
            dma((heads,)), dma((heads,)),
            dma((heads,)), dma((heads,)),
            dma((n,)), dma((n,)), dma((head_shards,)), dma((head_shards,)), dma((3,)),
            dma((heads,)), dma((heads,)),
        ],
        compiler_params=pltpu.CompilerParams(
            collective_id=1, has_side_effects=True, vmem_limit_bytes=60 * 2**20
        ),
    )


def local(teacher, student, weights):
    relations, block, t_columns = teacher.shape
    assert relations == 1
    heads = t_columns // TW
    n = lax.axis_size("seq")
    head_shards = lax.axis_size("head")
    assert n % heads == 0
    group = n // heads
    if group == 2 and heads & (heads - 1) == 0 and heads * SW % LANES == 0 and block % LANES == 0 and n * n * block * block <= 2**24:
        codes, peaks, loss = pair_call(heads, n, head_shards, block)(teacher[0], student[0], weights[None, :])
        student_grad, loss = decode_call(heads, block)(codes, peaks, loss)
        return (loss.reshape(()), student_grad[None])
    vmem = pl.BlockSpec(memory_space=pltpu.VMEM)
    dma = pltpu.SemaphoreType.DMA
    student_grad, loss = pl.pallas_call(
        functools.partial(kernel, heads, group, head_shards),
        out_shape=(
            jax.ShapeDtypeStruct((block, heads * SW), jnp.float32),
            jax.ShapeDtypeStruct((8, LANES), jnp.float32),
        ),
        in_specs=[vmem] * 3,
        out_specs=(vmem, vmem),
        scratch_shapes=[
            pltpu.VMEM((heads, block, LANES), jnp.bfloat16),
            pltpu.VMEM((8, block), jnp.float32),
            pltpu.VMEM((n * block, TW), jnp.bfloat16),
            pltpu.VMEM((n * block, LANES), jnp.bfloat16),
            pltpu.VMEM((heads, 8, block), jnp.float32),
            pltpu.VMEM((heads, 5, 8, block), jnp.float32),
            pltpu.VMEM((group, heads, 16, block), jnp.float32),
            pltpu.VMEM((heads, block, LANES), jnp.float32),
            pltpu.VMEM((heads, block, LANES), jnp.float32),
            pltpu.VMEM((n, 8, LANES), jnp.float32),
            pltpu.VMEM((head_shards, 8, LANES), jnp.float32),
            dma((heads,)), dma((heads,)), dma((heads,)),
            dma((heads, group)), dma((heads, group)),
            dma((n,)), dma((n,)), dma((heads,)),
            dma((group,)), dma((group,)),
            dma((heads,)), dma((heads,)),
            dma((n,)), dma((n,)), dma((head_shards,)), dma((head_shards,)),
        ],
        compiler_params=pltpu.CompilerParams(
            collective_id=0, has_side_effects=True, vmem_limit_bytes=60 * 2**20
        ),
    )(teacher[0], student[0], weights[None, :])
    return (loss[0, 0], student_grad[None])


def solution(mesh):
    return jax.shard_map(
        local,
        mesh=mesh,
        in_specs=(P(None, "seq", "head"), P(None, "seq", "head"), P("seq")),
        out_specs=(P(), P(None, "seq", "head")),
        check_vma=False,
    )
```

```python
import functools
import math

import jax
import jax.numpy as jnp
from jax import lax
from jax.experimental import pallas as pl
from jax.experimental.pallas import tpu as pltpu
from jax.sharding import PartitionSpec as P

TW = 256
SW = 112
LANES = 128
SPAN = 119.0
LOG2E = math.log2(math.e)
LN2 = math.log(2.0)
NT = (((1,), (1,)), ((), ()))


def dot_nt(a, b):
    return lax.dot_general(a, b, NT, preferred_element_type=jnp.float32)


def kernel(
    heads, group, head_shards, t_in, s_in, w_in, grad_out, loss_out,
    u_in, w_tile, t_all, u_all, w_all, state, norms, grads, landed, losses, sums,
    t_send, u_send, w_send, t_fwd, u_fwd, t_recv, u_recv, w_recv, n_send, n_recv, g_send, g_recv,
    l_send, l_recv, s_send, s_recv,
):
    n = heads * group
    block = t_in.shape[0]
    me = lax.axis_index("seq")
    shard = lax.axis_index("head")
    head = lax.div(me, group)
    member = lax.rem(me, group)
    unroll = math.gcd(n, 8)
    pair = math.gcd(heads, 2)
    t_scale = LOG2E / math.sqrt(TW)
    u_scale = LOG2E / math.sqrt(SW)

    def other_head(i):
        return lax.rem(head + i, heads)

    def source_head(i):
        return lax.rem(head + heads - i, heads)

    def other_member(i):
        return lax.rem(member + i, group)

    def remote(src, dst, send, recv, device):
        target = device if isinstance(device, dict) else {"seq": device}
        return pltpu.make_async_remote_copy(
            src_ref=src, dst_ref=dst, send_sem=send, recv_sem=recv,
            device_id=target, device_id_type=pl.DeviceIdType.MESH,
        )

    def rows(slot):
        return pl.ds(pl.multiple_of(slot * block, block), block)

    def columns(h):
        return pl.ds(pl.multiple_of(h * TW, TW), TW)

    barrier = pltpu.get_barrier_semaphore()
    for i in range(1, n):
        pl.semaphore_signal(barrier, inc=1, device_id={"seq": lax.rem(me + i, n)}, device_id_type=pl.DeviceIdType.MESH)
    for i in range(1, head_shards):
        pl.semaphore_signal(barrier, inc=1, device_id={"head": lax.rem(shard + i, head_shards)}, device_id_type=pl.DeviceIdType.MESH)
    for h in range(heads):
        u_in[h] = jnp.concatenate(
            [s_in[:, h * SW:(h + 1) * SW], jnp.zeros((block, LANES - SW), jnp.bfloat16)], axis=1
        )
    w_tile[...] = jnp.broadcast_to(w_in[...], w_tile.shape)
    pl.semaphore_wait(barrier, n + head_shards - 2)

    direct = []
    for i in range(1, heads):
        h = other_head(i)
        device = h * group + member
        direct += [
            remote(t_in.at[:, columns(h)], t_all.at[rows(me)], t_send.at[i], t_recv.at[me], device),
            remote(u_in.at[h], u_all.at[rows(me)], u_send.at[i], u_recv.at[me], device),
            remote(w_tile, w_all.at[head], w_send.at[i], w_recv.at[head], device),
        ]
    for copy in direct:
        copy.start()

    def forwards(i, slot, t_src, u_src):
        pairs = []
        for g in range(1, group):
            device = head * group + other_member(g)
            pairs += [
                remote(t_src, t_all.at[rows(slot)], t_fwd.at[i, g], t_recv.at[slot], device),
                remote(u_src, u_all.at[rows(slot)], u_fwd.at[i, g], u_recv.at[slot], device),
            ]
        return pairs

    def arrived(slot):
        remote(t_in.at[:, columns(0)], t_all.at[rows(slot)], t_send.at[0], t_recv.at[slot], me).wait_recv()
        remote(u_in.at[0], u_all.at[rows(slot)], u_send.at[0], u_recv.at[slot], me).wait_recv()

    for copy in forwards(0, me, t_in.at[:, columns(head)], u_in.at[head]):
        copy.start()
    t_all[rows(me), :] = t_in[:, columns(head)]
    u_all[rows(me), :] = u_in[head]
    w_all[head] = w_tile[...]

    low = jnp.full((8, block), -1e30, jnp.float32)
    zero = jnp.zeros((8, block), jnp.float32)
    for h in range(heads):
        for k, value in enumerate((low, zero, zero, low, zero)):
            state[h, k] = value

    def tile(row_head, key_pair):
        t_own = t_all[rows(row_head * group + member), :]
        u_own = u_all[rows(row_head * group + member), :]
        width = math.gcd(group, 2)
        parts = [(a, q) for a in range(pair) for q in range(width)]

        def step(j, carry):
            t_max, t_sum, t_cross, u_max, u_sum = carry
            for a, q in parts:
                keys = rows(source_head(key_pair * pair + a) * group + j * width + q)
                t_score = (dot_nt(t_all[keys, :], t_own) * t_scale).reshape(block // 8, 8, block)
                u_score = (dot_nt(u_all[keys, :], u_own) * u_scale).reshape(block // 8, 8, block)
                t_top = jnp.maximum(t_max, jnp.max(t_score, axis=0))
                u_top = jnp.maximum(u_max, jnp.max(u_score, axis=0))
                t_exp = jnp.exp2(t_score - t_top[None])
                u_exp = jnp.exp2(u_score - u_top[None])
                t_keep = jnp.exp2(t_max - t_top)
                u_keep = jnp.exp2(u_max - u_top)
                t_sum = t_sum * t_keep + jnp.sum(t_exp, axis=0)
                t_cross = t_cross * t_keep + jnp.sum(t_exp * (t_score - u_score), axis=0)
                u_sum = u_sum * u_keep + jnp.sum(u_exp, axis=0)
                t_max, u_max = t_top, u_top
            return t_max, t_sum, t_cross, u_max, u_sum

        carry = tuple(state[row_head, k] for k in range(5))
        carry = step(0, carry) if group == width else lax.fori_loop(0, group // width, step, carry)
        for k in range(5):
            state[row_head, k] = carry[k]

    def arrival(p, carry):
        for a in range(pair):
            i = p * pair + a
            h = source_head(i)
            slot = h * group + member

            @pl.when(i > 0)
            def _(i=i, slot=slot):
                arrived(slot)
                for copy in forwards(i, slot, t_all.at[rows(slot)], u_all.at[rows(slot)]):
                    copy.start()
        for a in range(pair):
            h = source_head(p * pair + a)
            for g in range(1, group):
                arrived(h * group + other_member(g))

        def one(j, carry):
            old = j < p * pair
            fresh = j - p * pair
            tile(
                source_head(jnp.where(old, j, p * pair + lax.rem(fresh, pair))),
                jnp.where(old, p, lax.div(fresh, pair)),
            )
            return carry

        return lax.fori_loop(0, p * pair + (p + 1) * pair, one, carry)

    lax.fori_loop(0, heads // pair, arrival, 0)
    for i in range(1, heads):
        remote(w_tile, w_all.at[source_head(i)], w_send.at[0], w_recv.at[source_head(i)], me).wait_recv()

    loss = jnp.zeros((1, block), jnp.float32)
    for i in range(heads):
        t_max, t_sum, t_cross, u_max, u_sum = (state[i, k] for k in range(5))
        t_top = jnp.max(t_max, axis=0, keepdims=True)
        u_top = jnp.max(u_max, axis=0, keepdims=True)
        t_keep = jnp.exp2(t_max - t_top)
        t_total = jnp.sum(t_sum * t_keep, axis=0, keepdims=True)
        t_mixed = jnp.sum(t_cross * t_keep, axis=0, keepdims=True)
        u_total = jnp.sum(u_sum * jnp.exp2(u_max - u_top), axis=0, keepdims=True)
        t_norm = t_top + jnp.log(t_total) * LOG2E
        u_norm = u_top + jnp.log(u_total) * LOG2E
        weight = w_all[i][:1, :]
        weight_log = jnp.log(weight) * LOG2E
        norms[member, i, 0:8, :] = jnp.broadcast_to(t_norm - weight_log, (8, block))
        norms[member, i, 8:16, :] = jnp.broadcast_to(u_norm - weight_log, (8, block))
        loss = loss + weight * (t_mixed / t_total - t_norm + u_norm)
    loss = jnp.sum(loss, axis=1, keepdims=True) * (LN2 / (heads * head_shards * block * n))
    losses[me] = jnp.broadcast_to(loss, losses.shape[1:])
    stats = [
        remote(norms.at[member], norms.at[member], n_send.at[g], n_recv.at[member], head * group + other_member(g))
        for g in range(1, group)
    ]
    for i in range(1, n):
        stats.append(remote(losses.at[me], losses.at[me], l_send.at[i], l_recv.at[me], lax.rem(me + i, n)))
    for copy in stats:
        copy.start()
    for g in range(1, group):
        m = other_member(g)
        remote(norms.at[m], norms.at[m], n_send.at[0], n_recv.at[m], me).wait_recv()

    def row_grad(i):
        slot = i * group + member
        t_own = t_all[rows(slot), :]
        u_own = u_all[rows(slot), :]

        def own_norm(first):
            tall = jnp.broadcast_to(norms[member, i, first:first + 1, :], (LANES, block)).T
            return jnp.concatenate([tall] * (block // LANES), axis=1)

        t_mine = own_norm(0)
        u_mine = own_norm(8)

        def step(j, total):
            for q in range(unroll):
                key = j * unroll + q
                keys = rows(key)
                key_head = lax.div(key, group)
                key_member = lax.rem(key, group)
                t_theirs = norms[key_member, key_head, 0:1, :]
                u_theirs = norms[key_member, key_head, 8:9, :]
                u_keys = u_all[keys, :]
                t_score = dot_nt(t_own, t_all[keys, :]) * t_scale
                u_score = dot_nt(u_own, u_keys) * u_scale
                row_part = jnp.exp2(u_score - u_mine) - jnp.exp2(t_score - t_mine)
                col_part = jnp.exp2(u_score - u_theirs) - jnp.exp2(t_score - t_theirs)
                mix = (row_part + col_part).astype(jnp.bfloat16)
                total = total + jnp.dot(mix, u_keys, preferred_element_type=jnp.float32)
            return total

        total = lax.fori_loop(0, n // unroll, step, jnp.zeros((block, LANES), jnp.float32))
        return total * (1.0 / math.sqrt(SW))

    def send_grad(i, h):
        return remote(grads.at[h], landed.at[head], g_send.at[h], g_recv.at[head], h * group + member)

    def grad_step(i, carry):
        h = other_head(i)
        grads[h] = row_grad(h)
        send_grad(i, h).start()
        return carry

    lax.fori_loop(1, heads, grad_step, 0)
    for i in range(1, n):
        peer = lax.rem(me + i, n)
        remote(losses.at[peer], losses.at[peer], l_send.at[0], l_recv.at[peer], me).wait_recv()
    sums[shard] = jnp.sum(losses[...], axis=0)
    shards = [
        remote(sums.at[shard], sums.at[shard], s_send.at[i], s_recv.at[shard], {"head": lax.rem(shard + i, head_shards)})
        for i in range(1, head_shards)
    ]
    for copy in shards:
        copy.start()
    landed[head] = row_grad(head)
    for i in range(1, head_shards):
        peer = lax.rem(shard + i, head_shards)
        remote(sums.at[peer], sums.at[peer], s_send.at[0], s_recv.at[peer], {"head": peer}).wait_recv()
    loss_out[...] = jnp.sum(sums[...], axis=0)

    for copy in direct + stats + shards:
        copy.wait_send()
    for i in range(heads):
        for copy in forwards(i, me, t_in.at[:, columns(0)], u_in.at[0]):
            copy.wait_send()
    for i in range(1, heads):
        send_grad(i, other_head(i)).wait_send()
    for h in range(heads):
        @pl.when(head != h)
        def _(h=h):
            remote(grads.at[h], landed.at[h], g_send.at[h], g_recv.at[h], me).wait_recv()
        grad_out[:, h * SW:(h + 1) * SW] = landed[h][:, :SW]


def pair_kernel(
    heads, head_shards, t_in, s_in, w_in, code_in, peak_in, loss_out,
    u_in, t_all, u_all, u_turn, w_all, t_raw, u_raw, t_exp, u_exp, t_refs, u_refs, t_top, u_top, cross,
    t_rows, u_rows, parts, landed_parts, code_out, peak_out, losses, sums,
    t_send, u_send, w_send, t_fwd, u_fwd, t_recv, u_recv, w_recv, p_send, p_recv, g_send, g_recv,
    l_send, l_recv, s_send, s_recv, own_sem, k_send, k_recv,
):
    group = 2
    n = heads * group
    block = t_in.shape[0]
    both = group * block
    me = lax.axis_index("seq")
    shard = lax.axis_index("head")
    head = lax.div(me, group)
    member = lax.rem(me, group)
    mate = head * group + 1 - member
    bits = (heads - 1).bit_length()
    t_scale = LOG2E / math.sqrt(TW)
    u_scale = LOG2E / math.sqrt(SW)

    half = heads // 2
    quarter = max(heads // 4, 1)

    def flip(i):
        i = jnp.int32(i)
        if heads >= 4:
            turned = half + lax.rem(i - half, 2) * quarter + lax.div(i - half, 2)
            i = i + lax.div(i, half) * (turned - i)
        out = 0
        for k in range(bits):
            out = out + lax.rem(lax.div(head, 2**k) + lax.div(jnp.int32(i), 2**k), 2) * 2**k
        return out

    def remote(src, dst, send, recv, device):
        target = device if isinstance(device, dict) else {"seq": device}
        return pltpu.make_async_remote_copy(
            src_ref=src, dst_ref=dst, send_sem=send, recv_sem=recv,
            device_id=target, device_id_type=pl.DeviceIdType.MESH,
        )

    def rows(slot):
        return pl.ds(pl.multiple_of(slot * block, block), block)

    def both_rows(h):
        return pl.ds(pl.multiple_of(h * both, both), both)

    def head_rows(h):
        return pl.ds(pl.multiple_of(h * SW, 16), SW)

    def columns(h):
        return pl.ds(pl.multiple_of(h * TW, TW), TW)

    barrier = pltpu.get_barrier_semaphore()
    for i in range(1, n):
        pl.semaphore_signal(barrier, inc=1, device_id={"seq": lax.rem(me + i, n)}, device_id_type=pl.DeviceIdType.MESH)
    for i in range(1, head_shards):
        pl.semaphore_signal(barrier, inc=1, device_id={"head": lax.rem(shard + i, head_shards)}, device_id_type=pl.DeviceIdType.MESH)
    for c in range(heads * SW // LANES):
        piece = s_in[:, c * LANES:(c + 1) * LANES].astype(jnp.float32)
        u_in[c * LANES:(c + 1) * LANES, :] = piece.T.astype(jnp.bfloat16)
    spare = lax.broadcasted_iota(jnp.int32, (LANES - SW, block), 0)
    ones = jnp.where(spare == 0, 1.0, 0.0).astype(jnp.bfloat16)
    for k in range(n):
        u_turn[k, SW:, :] = ones
    pl.semaphore_wait(barrier, n + head_shards - 2)

    direct = []
    for i in range(1, heads):
        h = flip(i)
        device = h * group + member
        direct += [
            remote(t_in.at[:, columns(h)], t_all.at[rows(me)], t_send.at[i], t_recv.at[me], device),
            remote(u_in.at[head_rows(h)], u_turn.at[me, pl.ds(0, SW)], u_send.at[i], u_recv.at[me], device),
            remote(w_in, w_all.at[head], w_send.at[i], w_recv.at[head], device),
        ]
    for copy in direct:
        copy.start()

    def forwards(i, slot, t_src, u_src):
        return [
            remote(t_src, t_all.at[rows(slot)], t_fwd.at[i], t_recv.at[slot], mate),
            remote(u_src, u_turn.at[slot, pl.ds(0, SW)], u_fwd.at[i], u_recv.at[slot], mate),
        ]

    def arrived(slot):
        remote(t_in.at[:, columns(0)], t_all.at[rows(slot)], t_send.at[0], t_recv.at[slot], mate).wait_recv()
        remote(u_in.at[head_rows(0)], u_turn.at[slot, pl.ds(0, SW)], u_send.at[0], u_recv.at[slot], mate).wait_recv()

    for copy in forwards(0, me, t_in.at[:, columns(head)], u_in.at[head_rows(head)]):
        copy.start()
    own_t = pltpu.make_async_copy(t_in.at[:, columns(head)], t_all.at[rows(me)], own_sem.at[0])
    own_t.start()
    u_turn[me, :SW, :] = u_in[head_rows(head), :]
    w_all[head] = w_in[...]
    lane = lax.broadcasted_iota(jnp.int32, (block, LANES), 1)

    def turn_u(slot):
        u_all[rows(slot), :] = jnp.where(lane < SW, u_turn[slot].astype(jnp.float32).T, 0.0).astype(jnp.bfloat16)

    for h in range(heads):
        t_top[h] = jnp.full((8, block), -1e30, jnp.float32)
        u_top[h] = jnp.full((8, block), -1e30, jnp.float32)
        cross[h] = jnp.zeros((8, block), jnp.float32)
        t_rows[h] = jnp.zeros((LANES, block), jnp.float32)
        u_rows[h] = jnp.zeros((LANES, block), jnp.float32)

    def fold(x, op):
        return op(x.reshape(x.shape[0] // 8, 8, block), axis=0)

    def unit(i, k):
        early = k < i
        return flip(jnp.where(early, i, k - i)), flip(jnp.where(early, k, i))

    def scores(i, k, b):
        own, key = unit(i, k)
        slot = own * group + member
        t = dot_nt(t_all[both_rows(key), :], t_all[rows(slot), :])
        u = jnp.dot(u_all[both_rows(key), :], u_turn[slot], preferred_element_type=jnp.float32)
        t_raw[b] = t
        u_raw[b] = u
        return fold(t, jnp.max), fold(u, jnp.max)

    def soften(i, k, b, peaks):
        own, key = unit(i, k)

        def side(raw_ref, peak, scale, top, refs, exps, out, with_cross):
            raw = raw_ref[b]
            old = top[own]
            new = jnp.maximum(old, jnp.max(peak, axis=0, keepdims=True))
            top[own] = new
            refs[own, pl.ds(key, 1), :] = new[:1] * scale
            value = jnp.exp2(raw * scale - new[:1] * scale).astype(jnp.bfloat16)
            keep = jnp.exp2((old - new) * scale)
            if with_cross:
                cross[own] = cross[own] * keep + fold(value.astype(jnp.float32) * raw, jnp.sum)
            total = out[own] * keep[:1]
            for q in range(group):
                piece = value[q * block:(q + 1) * block]
                exps[own, key * group + q] = piece
                total = total + jnp.dot(u_turn[key * group + q], piece, preferred_element_type=jnp.float32)
            out[own] = total

        side(t_raw, peaks[0], t_scale, t_top, t_refs, t_exp, t_rows, True)
        side(u_raw, peaks[1], u_scale, u_top, u_refs, u_exp, u_rows, False)

    turn_u(me)
    own_t.wait()
    arrived(head * group + 1 - member)
    turn_u(head * group + 1 - member)
    soften(0, 0, 0, scores(0, 0, 0))

    def arrival(i, carry):
        h = flip(i)
        slot = h * group + member
        other = h * group + 1 - member
        arrived(slot)
        for copy in forwards(i, slot, t_all.at[rows(slot)], u_turn.at[slot, pl.ds(0, SW)]):
            copy.start()
        turn_u(slot)

        def run(k, count, peaks):
            for z in range(count):
                ahead = scores(i, k + z + 1, (z + 1) % 2)
                soften(i, k + z, z % 2, peaks)
                peaks = ahead
            return peaks

        def whole():
            arrived(other)
            turn_u(other)

        def four(j, peaks):
            pl.when(j == lax.div(i - 1, 4))(whole)
            return run(4 * j, 4, peaks)

        def two(j, peaks):
            pl.when(i == 1)(whole)
            return run(2 * i - 2, 2, peaks)

        peaks = lax.fori_loop(0, lax.div(i, 2), four, scores(i, 0, 0))
        soften(i, 2 * i, 0, lax.fori_loop(0, lax.rem(i, 2), two, peaks))
        return carry

    lax.fori_loop(1, heads, arrival, 0)
    for i in range(1, heads):
        remote(w_in, w_all.at[flip(i)], w_send.at[0], w_recv.at[flip(i)], mate).wait_recv()

    loss = jnp.zeros((1, block), jnp.float32)
    for h in range(heads):
        weight = w_all[h][:1, :]
        t_sum = t_rows[h, SW:SW + 1, :]
        u_sum = u_rows[h, SW:SW + 1, :]
        t_norm = t_top[h][:1] * t_scale + jnp.log(t_sum) * LOG2E
        u_norm = u_top[h][:1] * u_scale + jnp.log(u_sum) * LOG2E
        own_u = u_turn[h * group + member].astype(jnp.float32)[:SW]
        seen = jnp.sum(own_u * t_rows[h, :SW, :], axis=0, keepdims=True) * u_scale
        mean = (jnp.sum(cross[h], axis=0, keepdims=True) * t_scale - seen) / t_sum
        loss = loss + weight * (mean - t_norm + u_norm)
        t_part = weight / t_sum
        u_part = weight / u_sum
        t_last = t_top[h][:1] * t_scale
        u_last = u_top[h][:1] * u_scale
        t_refs[h] = jnp.exp2(t_refs[h] - t_last) * t_part
        u_refs[h] = jnp.exp2(u_refs[h] - u_last) * u_part
        u_rows[h] = u_rows[h] * u_part - t_rows[h] * t_part
    loss = jnp.sum(loss, axis=1, keepdims=True) * (LN2 / (heads * head_shards * block * n))
    losses[me] = jnp.broadcast_to(loss, losses.shape[1:])
    stats = [
        remote(losses.at[me], losses.at[me], l_send.at[i], l_recv.at[me], lax.rem(me + i, n))
        for i in range(1, n)
    ]
    for copy in stats:
        copy.start()

    def column_parts(h):
        total = jnp.zeros((both, LANES), jnp.float32)
        for own in range(heads):
            t_part = t_exp[own, pl.ds(h * group, group)].astype(jnp.float32) * t_refs[own, pl.ds(h, 1), :]
            u_part = u_exp[own, pl.ds(h * group, group)].astype(jnp.float32) * u_refs[own, pl.ds(h, 1), :]
            mix = (u_part - t_part).astype(jnp.bfloat16).reshape(both, block)
            total = total + jnp.dot(
                mix, u_all[rows(own * group + member), :], preferred_element_type=jnp.float32
            )
        for q in range(group):
            parts[h, q] = total[q * block:(q + 1) * block].T[:SW]

    def swap(h):
        return remote(parts.at[h, 1 - member], landed_parts.at[h], p_send.at[h], p_recv.at[h], mate)

    def give(i, h):
        return remote(code_out.at[h], code_in.at[head], g_send.at[i], g_recv.at[head], h * group + member)

    def give_peak(i, h):
        return remote(peak_out.at[h], peak_in.at[head], k_send.at[i], k_recv.at[head], h * group + member)

    def finish(h):
        swap(h).wait_recv()
        return (parts[h, member] + u_rows[h, :SW, :] + landed_parts[h]) * (1.0 / math.sqrt(SW))

    def encode(h):
        grad = finish(h)
        peak = jnp.maximum(jnp.max(jnp.abs(grad), axis=0, keepdims=True), 1e-30)
        code_out[h] = jnp.exp2(grad * (SPAN / peak)).astype(jnp.bfloat16)
        peak_out[h] = peak

    def hand_over(i):
        h = flip(i)
        encode(h)
        give(i, h).start()
        give_peak(i, h).start()

    def step(j, carry):
        i = heads - 1 - j
        h = flip(i)
        column_parts(h)
        swap(h).start()

        @pl.when(j > 0)
        def _():
            hand_over(i + 1)
        return carry

    lax.fori_loop(0, heads, step, 0)
    for i in range(1, n):
        peer = lax.rem(me + i, n)
        remote(losses.at[peer], losses.at[peer], l_send.at[0], l_recv.at[peer], mate).wait_recv()
    sums[shard] = jnp.sum(losses[...], axis=0)
    shards = [
        remote(sums.at[shard], sums.at[shard], s_send.at[i], s_recv.at[shard], {"head": lax.rem(shard + i, head_shards)})
        for i in range(1, head_shards)
    ]
    for copy in shards:
        copy.start()
    encode(head)
    own_code = pltpu.make_async_copy(code_out.at[head], code_in.at[head], own_sem.at[1])
    own_code.start()
    own_peak = pltpu.make_async_copy(peak_out.at[head], peak_in.at[head], own_sem.at[2])
    own_peak.start()
    for i in range(1, head_shards):
        peer = lax.rem(shard + i, head_shards)
        remote(sums.at[peer], sums.at[peer], s_send.at[0], s_recv.at[peer], {"head": peer}).wait_recv()
    loss_out[0, 0] = jnp.max(jnp.sum(sums[...], axis=0))

    for copy in direct + stats + shards:
        copy.wait_send()
    for i in range(heads):
        for copy in forwards(i, me, t_in.at[:, columns(0)], u_in.at[head_rows(0)]):
            copy.wait_send()
        swap(flip(i)).wait_send()
    for i in range(1, heads):
        give(i, flip(i)).wait_send()
        give_peak(i, flip(i)).wait_send()
    own_code.wait()
    own_peak.wait()
    for i in range(1, heads):
        h = flip(i)
        remote(code_out.at[h], code_in.at[h], g_send.at[0], g_recv.at[h], mate).wait_recv()
        remote(peak_out.at[h], peak_in.at[h], k_send.at[0], k_recv.at[h], mate).wait_recv()

def decode_kernel(heads, codes, peaks, loss_in, grad_out, loss_out, flat):
    loss_out[0, 0] = loss_in[0, 0]
    ready = 0
    for h in range(heads):
        code = codes[h].astype(jnp.float32)
        flat[h * SW:(h + 1) * SW, :] = jnp.log(code) * (peaks[h] * (LOG2E / SPAN))
        while (ready + 1) * LANES <= (h + 1) * SW:
            columns = slice(ready * LANES, (ready + 1) * LANES)
            grad_out[:, columns] = flat[columns, :].T
            ready += 1


def decode_call(heads, block):
    smem = pl.BlockSpec(memory_space=pltpu.SMEM)
    return pl.pallas_call(
        functools.partial(decode_kernel, heads),
        grid=(block // LANES,),
        out_shape=(
            jax.ShapeDtypeStruct((block, heads * SW), jnp.float32),
            jax.ShapeDtypeStruct((1, 1), jnp.float32),
        ),
        in_specs=[
            pl.BlockSpec((heads, SW, LANES), lambda i: (0, 0, i)),
            pl.BlockSpec((heads, 1, LANES), lambda i: (0, 0, i)),
            smem,
        ],
        out_specs=(pl.BlockSpec((LANES, heads * SW), lambda i: (i, 0)), smem),
        scratch_shapes=[pltpu.VMEM((heads * SW, LANES), jnp.float32)],
    )


def pair_call(heads, n, head_shards, block):
    vmem = pl.BlockSpec(memory_space=pltpu.VMEM)
    dma = pltpu.SemaphoreType.DMA
    f32, bf16 = jnp.float32, jnp.bfloat16
    return pl.pallas_call(
        functools.partial(pair_kernel, heads, head_shards),
        out_shape=(
            jax.ShapeDtypeStruct((heads, SW, block), bf16),
            jax.ShapeDtypeStruct((heads, 1, block), f32),
            jax.ShapeDtypeStruct((1, 1), f32),
        ),
        in_specs=[pl.BlockSpec(memory_space=pl.ANY), vmem, vmem],
        out_specs=(
            pl.BlockSpec(memory_space=pl.ANY), pl.BlockSpec(memory_space=pl.ANY), pl.BlockSpec(memory_space=pltpu.SMEM)
        ),
        scratch_shapes=[
            pltpu.VMEM((heads * SW, block), bf16),
            pltpu.VMEM((n * block, TW), bf16),
            pltpu.VMEM((n * block, LANES), bf16),
            pltpu.VMEM((n, LANES, block), bf16),
            pltpu.VMEM((heads, 1, block), f32),
            pltpu.VMEM((2, 2 * block, block), f32),
            pltpu.VMEM((2, 2 * block, block), f32),
            pltpu.VMEM((heads, n, block, block), bf16),
            pltpu.VMEM((heads, n, block, block), bf16),
            pltpu.VMEM((heads, heads, block), f32),
            pltpu.VMEM((heads, heads, block), f32),
            pltpu.VMEM((heads, 8, block), f32),
            pltpu.VMEM((heads, 8, block), f32),
            pltpu.VMEM((heads, 8, block), f32),
            pltpu.VMEM((heads, LANES, block), f32),
            pltpu.VMEM((heads, LANES, block), f32),
            pltpu.VMEM((heads, 2, SW, block), f32),
            pltpu.VMEM((heads, SW, block), f32),
            pltpu.VMEM((heads, SW, block), bf16),
            pltpu.VMEM((heads, 1, block), f32),
            pltpu.VMEM((n, 8, LANES), f32),
            pltpu.VMEM((head_shards, 8, LANES), f32),
            dma((heads,)), dma((heads,)), dma((heads,)),
            dma((heads,)), dma((heads,)),
            dma((n,)), dma((n,)), dma((heads,)),
            dma((heads,)), dma((heads,)),
            dma((heads,)), dma((heads,)),
            dma((n,)), dma((n,)), dma((head_shards,)), dma((head_shards,)), dma((3,)),
            dma((heads,)), dma((heads,)),
        ],
        compiler_params=pltpu.CompilerParams(
            collective_id=1, has_side_effects=True, vmem_limit_bytes=60 * 2**20
        ),
    )


def local(teacher, student, weights):
    relations, block, t_columns = teacher.shape
    assert relations == 1
    heads = t_columns // TW
    n = lax.axis_size("seq")
    head_shards = lax.axis_size("head")
    assert n % heads == 0
    group = n // heads
    if group == 2 and heads & (heads - 1) == 0 and heads * SW % LANES == 0 and block % LANES == 0 and n * n * block * block <= 2**24:
        codes, peaks, loss = pair_call(heads, n, head_shards, block)(teacher[0], student[0], weights[None, :])
        student_grad, loss = decode_call(heads, block)(codes, peaks, loss)
        return (loss.reshape(()), student_grad[None])
    vmem = pl.BlockSpec(memory_space=pltpu.VMEM)
    dma = pltpu.SemaphoreType.DMA
    student_grad, loss = pl.pallas_call(
        functools.partial(kernel, heads, group, head_shards),
        out_shape=(
            jax.ShapeDtypeStruct((block, heads * SW), jnp.float32),
            jax.ShapeDtypeStruct((8, LANES), jnp.float32),
        ),
        in_specs=[vmem] * 3,
        out_specs=(vmem, vmem),
        scratch_shapes=[
            pltpu.VMEM((heads, block, LANES), jnp.bfloat16),
            pltpu.VMEM((8, block), jnp.float32),
            pltpu.VMEM((n * block, TW), jnp.bfloat16),
            pltpu.VMEM((n * block, LANES), jnp.bfloat16),
            pltpu.VMEM((heads, 8, block), jnp.float32),
            pltpu.VMEM((heads, 5, 8, block), jnp.float32),
            pltpu.VMEM((group, heads, 16, block), jnp.float32),
            pltpu.VMEM((heads, block, LANES), jnp.float32),
            pltpu.VMEM((heads, block, LANES), jnp.float32),
            pltpu.VMEM((n, 8, LANES), jnp.float32),
            pltpu.VMEM((head_shards, 8, LANES), jnp.float32),
            dma((heads,)), dma((heads,)), dma((heads,)),
            dma((heads, group)), dma((heads, group)),
            dma((n,)), dma((n,)), dma((heads,)),
            dma((group,)), dma((group,)),
            dma((heads,)), dma((heads,)),
            dma((n,)), dma((n,)), dma((head_shards,)), dma((head_shards,)),
        ],
        compiler_params=pltpu.CompilerParams(
            collective_id=0, has_side_effects=True, vmem_limit_bytes=60 * 2**20
        ),
    )(teacher[0], student[0], weights[None, :])
    return (loss[0, 0], student_grad[None])


def solution(mesh):
    return jax.shard_map(
        local,
        mesh=mesh,
        in_specs=(P(None, "seq", "head"), P(None, "seq", "head"), P("seq")),
        out_specs=(P(), P(None, "seq", "head")),
        check_vma=False,
    )
```
